32 devices in a mesh: img: 2 (over x), sub: 16 (over z, y, core).
Axes of the slice: x: 2, y: 2, z: 4, core: 2. Of those that a mesh axis runs over, the one named last changes fastest.
Arguments:
- sub_images: float32 [2, 512, 4096], P(None, ('img', 'sub')), parts along dimension 1, may hold values from -6 to 6
- shift_table: int32 [4, 16, 2, 8], P(None, 'sub'), may hold values from -256 to 256
- phase_table: float32 [4, 16, 2, 8], P(None, 'sub'), may hold values from -3.140625 to 3.140625
- offset_table: int32 [4, 16, 2, 16], P(None, 'sub'), may hold values from 0 to 4
- weight_table: float32 [4, 16, 2, 4, 16], P(None, 'sub'), may hold values from -2 to 2
Outputs:
- turned_image: float32 [2, 8192, 256], P(None, ('img', 'sub')), parts along dimension 1
The draws below stay inside these ranges and needn't reach their ends.
There are 2 independent parts, one for each index of `img`. The reference program is written for one: setup_inputs(seed, part) draws one part's arguments, and reference() takes and returns one part's arrays. A program takes and returns all parts, laid end to end along the dimension named above; an argument that names none is the same for every part. Nothing has to cross between parts.
All inputs are finite; a program needn't handle non-finite values.
Results may differ from the reference program's by a relative error of at most 0.0003.
Values sent between devices are 32-bit elements; how exact they have to be, the bound alone decides.
A program may use at most 64 MiB of HBM per device.

```python
import math
import jax
import jax.numpy as jnp
from jax import lax

B = 16
R = 4096
TAPS = 4
HALF = 8
LEVELS = 4
BEAMS = 256
N_SUB = 16


def with_ends(values, stream_key, least, high):
    extent = values.shape
    index_at = [jax.random.randint(jax.random.fold_in(stream_key, axis), (), 0, extent[axis]) for axis in range(len(extent))]
    values = values.at[tuple(index_at)].set(least)
    longest = extent.index(max(extent))
    index_at[longest] = (index_at[longest] + 1) % extent[longest]
    return values.at[tuple(index_at)].set(high)


def block_scale(key, extent, shards, least, high):
    def one(axis_at, parts):
        heights = jax.random.uniform(jax.random.fold_in(jax.random.fold_in(key, 6), axis_at), (parts,), jnp.float32, least / len(shards), high / len(shards))
        return jnp.repeat(jnp.exp(heights), extent[axis_at] // parts).reshape((-1,) + (1,) * (len(extent) - axis_at - 1))

    loudness = one(*shards[0])
    for cut in shards[1:]:
        loudness = loudness * one(*cut)
    return loudness


def scatter_about(own_key, dims, scale, reach, pieces=(), kind=jnp.bfloat16):
    result = jax.random.normal(own_key, dims, jnp.float32) * scale
    if len(pieces) > 0:
        result = block_scale(own_key, dims, pieces, -0.22, 0.18) * result
    return jnp.clip(result, min=-reach, max=reach).astype(kind)


def setup_inputs(seed: int = 0, part: int = 0) -> dict:
    streams_of = jax.random.split(jax.random.key(seed), 6)
    part_keys = jax.random.split(jax.random.fold_in(streams_of[5], part), 6)
    return {
        "sub_images": scatter_about(part_keys[0], (2, BEAMS, R), 1.0, 6.0, ((1, 16),), jnp.float32),
        "shift_table": with_ends(jax.random.randint(streams_of[1], (LEVELS, N_SUB, 2, HALF), -256, 257), jax.random.fold_in(streams_of[1], 1), -256, 256).astype(jnp.int32),
        "phase_table": jnp.clip(jax.random.uniform(streams_of[2], (LEVELS, N_SUB, 2, HALF), jnp.float32, -3.140625, 3.140625), -3.140625, 3.140625),
        "offset_table": with_ends(jax.random.randint(streams_of[3], (LEVELS, N_SUB, 2, B), 0, HALF - TAPS + 1), jax.random.fold_in(streams_of[3], 1), 0, HALF - TAPS).astype(jnp.int32),
        "weight_table": scatter_about(streams_of[4], (LEVELS, N_SUB, 2, TAPS, B), (2 * TAPS) ** -0.5, 2.0, ((1, 16),), jnp.float32),
    }


def signed_frequency(length):
    indices = jnp.arange(length, dtype=jnp.int32)
    return ((indices + length // 2) % length) - length // 2


def reference(sub_images, shift_table, phase_table, offset_table, weight_table):
    current = sub_images.reshape(2, N_SUB, B, R)
    indices = jnp.arange(N_SUB, dtype=jnp.int32)
    frequency = signed_frequency(R)
    columns = jnp.arange(HALF, dtype=jnp.int32)
    for level_idx in range(LEVELS):
        partner = indices ^ (1 << level_idx)
        side_bit = (indices >> level_idx) & 1
        halves = current.reshape(2, N_SUB, 2, HALF, R)
        kept_half = halves[:, indices, side_bit]
        arrived = halves[:, partner, side_bit]
        children = jnp.stack([kept_half, arrived], axis=2)
        complex_in = children[0] + 1j * children[1]
        spectrum = jnp.fft.fft(complex_in, axis=-1)
        shifts = shift_table[level_idx]
        turns = ((frequency[None, None, None, :] * shifts[..., None]) % (4 * R)).astype(phase_table.dtype)
        angles = phase_table[level_idx][..., None] - turns * (2.0 * math.pi / (4 * R))
        spectrum = spectrum * (jnp.cos(angles) + 1j * jnp.sin(angles))
        moved = jnp.fft.ifft(spectrum, axis=-1)
        offsets = offset_table[level_idx]
        weights = weight_table[level_idx]
        stencil = jnp.zeros((N_SUB, 2, B, HALF), weight_table.dtype)
        for tap_idx in range(TAPS):
            hits = (columns[None, None, None, :] == offsets[..., None] + tap_idx).astype(weight_table.dtype)
            stencil = stencil + weights[:, :, tap_idx, :, None] * hits
        real_part = jnp.einsum("icjm,icmr->ijr", stencil, jnp.real(moved), precision=lax.Precision.HIGHEST)
        imag_part = jnp.einsum("icjm,icmr->ijr", stencil, jnp.imag(moved), precision=lax.Precision.HIGHEST)
        current = jnp.stack([real_part, imag_part])
    return jnp.transpose(current.reshape(2, N_SUB * B, R), (0, 2, 1))
```

```python
import functools
import math

import jax
import jax.numpy as jnp
import numpy as np
from jax import lax
from jax.experimental import pallas as pl
from jax.experimental.pallas import tpu as pltpu
from jax.sharding import PartitionSpec as P

LANES = 128
CHUNK = 8
F32 = jnp.float32
BF16 = jnp.bfloat16


def split(values):
    high = values.astype(BF16)
    low = (values - high.astype(F32)).astype(BF16)
    return high, low


def dot(left, right):
    return jnp.dot(left, right, preferred_element_type=F32)


def times_constant(pair, constant):
    real_part, imag_part = pair
    c, s = constant.real, constant.imag
    if abs(s) < 1e-12:
        return pair if c > 0 else (-real_part, -imag_part)
    if abs(c) < 1e-12:
        return (-imag_part, real_part) if s > 0 else (imag_part, -real_part)
    if abs(abs(c) - abs(s)) < 1e-12:
        h = abs(c)
        a = real_part if c > 0 else -real_part
        b = imag_part if s > 0 else -imag_part
        e = real_part if s > 0 else -real_part
        f = imag_part if c > 0 else -imag_part
        return (a - b) * h, (e + f) * h
    return real_part * c - imag_part * s, real_part * s + imag_part * c


def butterflies(rows, direction):
    n = len(rows)
    if n == 1:
        return rows
    even = butterflies(rows[0::2], direction)
    odd = butterflies(rows[1::2], direction)
    first, second = [], []
    for k in range(n // 2):
        angle = direction * 2.0 * math.pi * k / n
        tr, ti = times_constant(odd[k], complex(math.cos(angle), math.sin(angle)))
        er, ei = even[k]
        first.append((er + tr, ei + ti))
        second.append((er - tr, ei - ti))
    return first + second


def kernel(cfg, x_hbm, shift_hbm, phase_hbm, offset_hbm, weight_hbm, wf_hbm, wi_hbm, tw_hbm, *refs):
    outs, refs = refs[: cfg["outs"]], refs[cfg["outs"] :]
    (x_ref, shift_ref, phase_ref, offset_ref, weight_ref, wf_ref, wi_ref, tw_ref,
     field, state, landed, raw, tables, merge, sendbuf, gathered, card, cards, last,
     load_sem, level_send, level_recv, turn_send, turn_recv, card_send, card_recv) = refs
    n, levels, outer, beams, chunks = cfg["n"], cfg["levels"], cfg["outer"], cfg["beams"], cfg["chunks"]
    per, groups, width, rows = cfg["per"], cfg["groups"], cfg["width"], cfg["rows"]
    half = beams // 2
    size = outer // chunks
    extent = size * beams
    taps = cfg["taps"]
    total = outer * LANES
    final = levels - 1
    me = lax.axis_index("sub")

    def bit(level):
        return (me // (1 << level)) % 2

    def across(mask):
        other = me
        for level in range(levels):
            if mask >> level & 1:
                other = other + (1 - 2 * bit(level)) * (1 << level)
        return other

    pairs = [(x_hbm.at[:, pl.ds(g * 8, 8)], x_ref.at[:, pl.ds(g * 8, 8)]) for g in range(beams // 8)]
    pairs += [(tw_hbm, tw_ref), (wf_hbm, wf_ref), (shift_hbm, shift_ref), (phase_hbm, phase_ref),
              (offset_hbm, offset_ref), (weight_hbm, weight_ref), (wi_hbm, wi_ref)]
    loads = [pltpu.make_async_copy(src, dst, load_sem.at[i]) for i, (src, dst) in enumerate(pairs)]
    for load in loads:
        load.start()

    barrier = pltpu.get_barrier_semaphore()
    for mask in range(1, n):
        pl.semaphore_signal(barrier, inc=1, device_id={"sub": across(mask)}, device_id_type=pl.DeviceIdType.MESH)

    later = beams // 8
    for g in range(beams // 8):
        loads[g].wait()
        if g == 0:
            loads[later].wait()
        lines = [
            tuple(x_ref[p, g * 8 : g * 8 + 8, q * LANES : (q + 1) * LANES] for p in range(2)) for q in range(outer)
        ]
        for k, (re, im) in enumerate(butterflies(lines, -1)):
            tr, ti = tw_ref[0, k : k + 1, :], tw_ref[1, k : k + 1, :]
            field[k, g * 8 : g * 8 + 8, :LANES] = re * tr + im * ti
            field[k, g * 8 : g * 8 + 8, LANES:] = im * tr - re * ti

    def card_copy(v):
        there = (me + v) % n
        return pltpu.make_async_remote_copy(
            src_ref=card, dst_ref=cards.at[me], send_sem=card_send.at[v], recv_sem=card_recv.at[v],
            device_id={"sub": there}, device_id_type=pl.DeviceIdType.MESH,
        )

    def card_arrival(v):
        return pltpu.make_async_remote_copy(
            src_ref=card, dst_ref=cards.at[(me + n - v) % n], send_sem=card_send.at[v], recv_sem=card_recv.at[v],
            device_id={"sub": (me + n - v) % n}, device_id_type=pl.DeviceIdType.MESH,
        )

    def write_card():
        for load in loads[later + 2 : later + 6]:
            load.wait()
        place = lax.broadcasted_iota(jnp.int32, (half, beams), 0)
        blocks = []
        for child in range(2):
            first = offset_ref[final, 0, child : child + 1, :]
            block = jnp.zeros((half, beams), F32)
            for t in range(taps):
                block = block + jnp.where(place == first + t, weight_ref[final, 0, child, t : t + 1, :], 0.0)
            blocks.append(block)
        eye = lax.broadcasted_iota(jnp.int32, (half, half), 0) == lax.broadcasted_iota(jnp.int32, (half, half), 1)
        for row in (shift_ref[final, 0, 1:2, :].astype(F32), phase_ref[final, 0, 1:2, :]):
            blocks.append(jnp.sum(jnp.where(eye, row, 0.0), axis=1, keepdims=True))
        blocks.append(jnp.zeros((half, LANES - 2 * beams - 2), F32))
        card[...] = jnp.concatenate(blocks, axis=1)

    def prepare():
        loads[later + 6].wait()
        raw[...] = jnp.zeros_like(raw)
        count = 6 + 2 * taps
        for level in range(levels):
            at = level * count
            raw[at : at + 2, :half] = shift_ref[level, 0].astype(F32)
            raw[at + 2 : at + 4, :half] = phase_ref[level, 0]
            raw[at + 4 : at + 6, :beams] = offset_ref[level, 0].astype(F32)
            for child in range(2):
                raw[at + 6 + child * taps : at + 6 + (child + 1) * taps, :beams] = weight_ref[level, 0, child]
        blocks = [raw[i * LANES : (i + 1) * LANES].T for i in range(raw.shape[0] // LANES)]

        def column(level, row, extent):
            at = level * count + row
            return blocks[at // LANES][:extent, at % LANES : at % LANES + 1]

        lane = lax.broadcasted_iota(jnp.int32, (beams, LANES), 1)
        wide = lax.broadcasted_iota(jnp.int32, (beams, extent), 1)
        mask = (
            lax.broadcasted_iota(jnp.int32, (extent, extent), 0) // beams
            == lax.broadcasted_iota(jnp.int32, (extent, extent), 1) // beams
        )
        slot = wide % beams
        second = slot >= half
        place = (slot % half).astype(F32)
        card_arrival(n // 2).wait_recv()
        other = cards[(me + n // 2) % n]
        for level in range(levels):
            shifts = [column(level, child, half) for child in range(2)]
            phases = [column(level, 2 + child, half) for child in range(2)]
            if level == final:
                own_first = bit(final) == 0
                a, b = shifts[0], other[:, 2 * beams : 2 * beams + 1]
                shifts = [jnp.where(own_first, a, b), jnp.where(own_first, b, a)]
                a, b = phases[0], other[:, 2 * beams + 1 : 2 * beams + 2]
                phases = [jnp.where(own_first, a, b), jnp.where(own_first, b, a)]
            shift = jnp.concatenate(shifts, axis=0).astype(jnp.int32)
            phase = jnp.concatenate(phases, axis=0)
            signed = jnp.where(lane >= LANES // 2, lane - LANES, lane) * outer
            unit = 2.0 * math.pi / (4 * total)
            coarse = phase - ((signed * shift) & (4 * total - 1)).astype(F32) * unit
            fine = ((lane * shift) & (4 * total - 1)).astype(F32) * (-unit)
            tables[level, 0] = jnp.cos(coarse)
            tables[level, 1] = jnp.sin(coarse)
            tables[level, 2] = jnp.cos(fine)
            tables[level, 3] = jnp.sin(fine)
            if level == final:
                continue
            first = jnp.where(second, column(level, 5, beams), column(level, 4, beams))
            block = jnp.zeros((beams, extent), F32)
            for t in range(taps):
                weight = jnp.where(second, column(level, 6 + taps + t, beams), column(level, 6 + t, beams))
                block = block + jnp.where(place == first + t, weight, 0.0)
            tiled = jnp.concatenate([block] * size, axis=0)
            high, low = split(jnp.where(mask, tiled, 0.0))
            merge[level, 0] = high
            merge[level, 1] = low

    def level_copy(level, c):
        return pltpu.make_async_remote_copy(
            src_ref=state.at[level, c, 1 - bit(level)],
            dst_ref=landed.at[level, c],
            send_sem=level_send.at[level, c],
            recv_sem=level_recv.at[level, c],
            device_id={"sub": across(1 << level)},
            device_id_type=pl.DeviceIdType.MESH,
        )

    def publish(level, c, values):
        values = values.reshape(size, 2, half, 2 * LANES)
        for h in range(2):
            state[level, c, h] = values[:, h]
        level_copy(level, c).start()

    def transformed(values, w_ref):
        high, low = split(values)
        return dot(high, w_ref[0]) + dot(low, w_ref[0]) + dot(high, w_ref[1])

    loads[later + 1].wait()
    for c in range(chunks):
        values = transformed(field[c * size : (c + 1) * size].reshape(size * beams, 2 * LANES), wf_ref)
        if c == 0:
            write_card()
            pl.semaphore_wait(barrier, n - 1)
        publish(0, c, values)
    for v in range(1, n):
        card_copy(v).start()
    prepare()

    def turned(level, c, both):
        fr, fi = [], []
        cr, ci = tables[level, 0], tables[level, 1]
        sr, si = tables[level, 2], tables[level, 3]
        for k in range(c * size, (c + 1) * size):
            ar, ai = sr[:, k : k + 1], si[:, k : k + 1]
            fr.append(cr * ar - ci * ai)
            fi.append(cr * ai + ci * ar)
        fr, fi = jnp.stack(fr), jnp.stack(fi)
        zr, zi = both[..., :LANES], both[..., LANES:]
        return jnp.concatenate([zr * fr - zi * fi, zr * fi + zi * fr], axis=-1).reshape(size * beams, 2 * LANES)

    def stage(level, c):
        level_copy(level, c).wait_recv()
        kept = state[level, c, bit(level)]
        both = jnp.concatenate([kept, landed[level, c]], axis=1)
        high, low = split(turned(level, c, both))
        values = dot(merge[level, 0], high) + dot(merge[level, 0], low) + dot(merge[level, 1], high)
        if level + 1 < final:
            publish(level + 1, c, values)
            return
        values = turned(final, c, values.reshape(size, beams, 2 * LANES))
        back = transformed(values, wi_ref).reshape(size, beams, 2 * LANES)
        for k in range(size):
            at = c * size + k
            tr, ti = tw_ref[0, at : at + 1, :], tw_ref[1, at : at + 1, :]
            re, im = back[k, :, :LANES], back[k, :, LANES:]
            field[at, :, :LANES] = re * tr - im * ti
            field[at, :, LANES:] = im * tr + re * ti

    def turn_order(at):
        level, c = at
        return (2.1 * level + c if level else c - chunks, level)

    for level, c in sorted(((a, b) for a in range(final) for b in range(chunks)), key=turn_order):
        stage(level, c)

    for g in range(beams // 8):
        at = slice(g * 8, g * 8 + 8)
        lines = [(field[k, at, :LANES], field[k, at, LANES:]) for k in range(outer)]
        for q, pair in enumerate(butterflies(lines, 1)):
            for p in range(2):
                if groups == 1:
                    sendbuf[q // per, q % per, p, at] = pair[p]
                else:
                    field[q, at, p * LANES : (p + 1) * LANES] = pair[p]
    if groups > 1:
        for q in range(outer):
            for p in range(2):
                line = field[q, :, p * LANES : (p + 1) * LANES]
                for g in range(groups):
                    parts = [line[s * rows : (s + 1) * rows, g * width : (g + 1) * width] for s in range(groups)]
                    sendbuf[q * groups + g, 0, p] = jnp.concatenate(parts, axis=1)

    def turn_copy(v):
        there = (me + v) % n
        return pltpu.make_async_remote_copy(
            src_ref=sendbuf.at[there], dst_ref=gathered.at[me], send_sem=turn_send.at[v], recv_sem=turn_recv.at[v],
            device_id={"sub": there}, device_id_type=pl.DeviceIdType.MESH,
        )

    def turn_arrival(v):
        here = (me + n - v) % n
        return pltpu.make_async_remote_copy(
            src_ref=sendbuf.at[here], dst_ref=gathered.at[here], send_sem=turn_send.at[v], recv_sem=turn_recv.at[v],
            device_id={"sub": here}, device_id_type=pl.DeviceIdType.MESH,
        )

    for v in range(1, n):
        turn_copy(v).start()
    gathered[me] = sendbuf[me]
    cards[me] = card[...]
    for v in range(1, n):
        if v != n // 2:
            card_arrival(v).wait_recv()
    families = n // 16
    if groups == 1:
        lane = lax.broadcasted_iota(jnp.int32, (half, LANES), 1)
        for h in range(2):
            for g in range(families):
                tiles = []
                for side in range(2):
                    for f in range(8):
                        values = cards[h * (n // 2) + g * 8 + f]
                        child = side ^ h
                        moved = pltpu.roll(values, (f - child) * beams % LANES, 1)
                        tiles.append(jnp.where((lane >= f * beams) & (lane < (f + 1) * beams), moved, 0.0))
                high, low = split(jnp.concatenate(tiles, axis=0))
                last[h, g, 0] = high
                last[h, g, 1] = low
    for level in range(final):
        for c in range(chunks):
            level_copy(level, c).wait_send()
    for v in range(1, n):
        card_copy(v).wait_send()
    for v in range(1, n):
        turn_arrival(v).wait_recv()
    if groups == 1:
        for r in range(per):
            for p in range(2):
                for h in range(2):
                    for g in range(families):
                        sides = [
                            gathered[at : at + 8, r, p, h * half : (h + 1) * half].reshape(LANES // 2, LANES)
                            for at in (g * 8, n // 2 + g * 8)
                        ]
                        high, low = split(jnp.concatenate(sides, axis=0).T)
                        value = dot(high, last[h, g, 0]) + dot(low, last[h, g, 0]) + dot(high, last[h, g, 1])
                        at = (h * families + g) * LANES
                        outs[0][p, r * LANES : (r + 1) * LANES, at : at + LANES] = value
    else:
        for p in range(2):
            outs[0][:, :, p] = gathered[:, :, p]
        outs[1][...] = cards[...]
    for v in range(1, n):
        turn_copy(v).wait_send()


def real_form(length, direction, factor):
    index = np.arange(length)
    turns = (index[:, None] * index[None, :] % length) * (direction * 2.0 * np.pi / length)
    c, s = np.cos(turns) * factor, np.sin(turns) * factor
    full = np.block([[c, s], [-s, c]]).astype(np.float32)
    high = np.asarray(full, dtype=jnp.bfloat16)
    low = np.asarray(full - high.astype(np.float32), dtype=jnp.bfloat16)
    return np.stack([high, low])


def body(n, sub_images, shift_table, phase_table, offset_table, weight_table):
    beams, bins = sub_images.shape[1], sub_images.shape[2]
    levels, taps = shift_table.shape[0], weight_table.shape[3]
    outer = bins // LANES
    share = bins // n
    per = max(1, share // LANES)
    groups = max(1, LANES // share)
    size = CHUNK
    chunks = outer // size
    rows = beams // groups
    cfg = dict(n=n, levels=levels, outer=outer, beams=beams, chunks=chunks, per=per, groups=groups,
               width=min(share, LANES), rows=rows, taps=taps)
    turns = np.arange(outer)[:, None] * np.arange(LANES)[None, :] * (2.0 * np.pi / bins)
    twiddle = np.stack([np.cos(turns), np.sin(turns)]).astype(np.float32)
    half = beams // 2
    shapes = [(2, per * LANES, n * beams)] if groups == 1 else [(n, per, 2, rows, LANES), (n, half, LANES)]
    cfg["outs"] = len(shapes)
    vmem = pl.BlockSpec(memory_space=pltpu.VMEM)
    operands = (
        sub_images, shift_table, phase_table, offset_table, weight_table, jnp.asarray(real_form(LANES, -1, 1.0)),
        jnp.asarray(real_form(LANES, 1, 1.0 / bins)), jnp.asarray(twiddle),
    )
    result = pl.pallas_call(
        functools.partial(kernel, cfg),
        name="merges",
        out_shape=[jax.ShapeDtypeStruct(shape, F32) for shape in shapes],
        in_specs=[pl.BlockSpec(memory_space=pltpu.HBM)] * 8,
        out_specs=[vmem] * len(shapes),
        scratch_shapes=[
            *[pltpu.VMEM(a.shape, a.dtype) for a in operands],
            pltpu.VMEM((outer, beams, 2 * LANES), F32),
            pltpu.VMEM((levels - 1, chunks, 2, size, beams // 2, 2 * LANES), F32),
            pltpu.VMEM((levels - 1, chunks, size, beams // 2, 2 * LANES), F32),
            pltpu.VMEM((-(-levels * (6 + 2 * taps) // LANES) * LANES, LANES), F32),
            pltpu.VMEM((levels, 4, beams, LANES), F32),
            pltpu.VMEM((levels - 1, 2, size * beams, size * beams), BF16),
            pltpu.VMEM((n, per, 2, rows, LANES), F32),
            pltpu.VMEM((n, per, 2, rows, LANES), F32),
            pltpu.VMEM((half, LANES), F32),
            pltpu.VMEM((n, half, LANES), F32),
            pltpu.VMEM((2, n // 16, 2, LANES, LANES), BF16),
            pltpu.SemaphoreType.DMA((beams // 8 + 7,)),
            pltpu.SemaphoreType.DMA((levels - 1, chunks)),
            pltpu.SemaphoreType.DMA((levels - 1, chunks)),
            *[pltpu.SemaphoreType.DMA((n,))] * 4,
        ],
        compiler_params=pltpu.CompilerParams(
            collective_id=0, has_side_effects=True, vmem_limit_bytes=66400000
        ),
    )(*operands)
    if groups == 1:
        return result[0]
    pieces = result[0].reshape(n, 2, rows, groups, share).transpose(1, 4, 0, 3, 2)
    pieces = pieces.reshape(2, share, 2, n // 2, 2, half)
    blocks = result[1][:, :, : 2 * beams].reshape(2, n // 2, half, 2, beams)
    sums = []
    for h in range(2):
        total = 0.0
        for child in range(2):
            total = total + jnp.einsum(
                "pqim,imj->pqij", pieces[:, :, h ^ child, :, h], blocks[h, :, :, child], precision=lax.Precision.HIGHEST
            )
        sums.append(total)
    return jnp.stack(sums, axis=2).reshape(2, share, n * beams)


def solution(mesh):
    placed = (
        P(None, ("img", "sub"), None),
        P(None, "sub", None, None),
        P(None, "sub", None, None),
        P(None, "sub", None, None),
        P(None, "sub", None, None, None),
    )
    return jax.shard_map(
        functools.partial(body, mesh.shape["sub"]),
        mesh=mesh, in_specs=placed, out_specs=P(None, ("img", "sub"), None), check_vma=False,
    )
```

```python
import functools
import math

import jax
import jax.numpy as jnp
import numpy as np
from jax import lax
from jax.experimental import pallas as pl
from jax.experimental.pallas import tpu as pltpu
from jax.sharding import PartitionSpec as P

LANES = 128
CHUNKS = (1, 1, 2, 2, 1, 1)
VMEM = 67043328 - (3 << 16)
F32 = jnp.float32
BF16 = jnp.bfloat16


def split(values):
    high = values.astype(BF16)
    low = (values - high.astype(F32)).astype(BF16)
    return high, low


def dot(left, right):
    return jnp.dot(left, right, preferred_element_type=F32)


def times_constant(pair, constant):
    real_part, imag_part = pair
    c, s = constant.real, constant.imag
    if abs(s) < 1e-12:
        return pair if c > 0 else (-real_part, -imag_part)
    if abs(c) < 1e-12:
        return (-imag_part, real_part) if s > 0 else (imag_part, -real_part)
    if abs(abs(c) - abs(s)) < 1e-12:
        h = abs(c)
        a = real_part if c > 0 else -real_part
        b = imag_part if s > 0 else -imag_part
        e = real_part if s > 0 else -real_part
        f = imag_part if c > 0 else -imag_part
        return (a - b) * h, (e + f) * h
    return real_part * c - imag_part * s, real_part * s + imag_part * c


def butterflies(rows, direction):
    n = len(rows)
    if n == 1:
        return rows
    even = butterflies(rows[0::2], direction)
    odd = butterflies(rows[1::2], direction)
    first, second = [], []
    for k in range(n // 2):
        angle = direction * 2.0 * math.pi * k / n
        tr, ti = times_constant(odd[k], complex(math.cos(angle), math.sin(angle)))
        er, ei = even[k]
        first.append((er + tr, ei + ti))
        second.append((er - tr, ei - ti))
    return first + second


def kernel(cfg, x_hbm, shift_hbm, phase_hbm, offset_hbm, weight_hbm, wf_hbm, wi_hbm, tw_hbm, *refs):
    gathered, more, refs = refs[0], refs[1], refs[2:]
    (x_ref, shift_ref, phase_ref, offset_ref, weight_ref, wf_ref, wi_ref, tw_ref,
     field, state, landed, raw, columns, tables, merge, sendbuf, card, cards,
     load_sem, level_send, level_recv, turn_send, turn_recv, card_send, card_recv) = refs
    n, levels, outer, beams, sizes = cfg["n"], cfg["levels"], cfg["outer"], cfg["beams"], cfg["sizes"]
    per, groups, width, rows = cfg["per"], cfg["groups"], cfg["width"], cfg["rows"]
    half = beams // 2
    chunks = len(sizes)
    starts = [sum(sizes[:c]) for c in range(chunks)]
    most = max(sizes)
    extent = most * beams
    taps = cfg["taps"]
    total = outer * LANES
    final = levels - 1
    me = lax.axis_index("sub")

    def bit(level):
        return (me // (1 << level)) % 2

    def across(mask):
        other = me
        for level in range(levels):
            if mask >> level & 1:
                other = other + (1 - 2 * bit(level)) * (1 << level)
        return other

    pairs = [(x_hbm.at[:, pl.ds(g * 8, 8)], x_ref.at[:, pl.ds(g * 8, 8)]) for g in range(beams // 8)]
    pairs += [(tw_hbm, tw_ref), (wf_hbm, wf_ref), (shift_hbm, shift_ref), (phase_hbm, phase_ref),
              (offset_hbm, offset_ref), (weight_hbm, weight_ref), (wi_hbm, wi_ref)]
    loads = [pltpu.make_async_copy(src, dst, load_sem.at[i]) for i, (src, dst) in enumerate(pairs)]
    for load in loads:
        load.start()

    barrier = pltpu.get_barrier_semaphore()
    for mask in range(1, n):
        pl.semaphore_signal(barrier, inc=1, device_id={"sub": across(mask)}, device_id_type=pl.DeviceIdType.MESH)

    later = beams // 8
    for g in range(beams // 8):
        loads[g].wait()
        if g == 0:
            loads[later].wait()
        lines = [
            tuple(x_ref[p, g * 8 : g * 8 + 8, q * LANES : (q + 1) * LANES] for p in range(2)) for q in range(outer)
        ]
        for k, (re, im) in enumerate(butterflies(lines, -1)):
            tr, ti = tw_ref[0, k : k + 1, :], tw_ref[1, k : k + 1, :]
            field[k, g * 8 : g * 8 + 8, :LANES] = re * tr + im * ti
            field[k, g * 8 : g * 8 + 8, LANES:] = im * tr - re * ti

    def card_copy(v):
        there = (me + v) % n
        return pltpu.make_async_remote_copy(
            src_ref=card, dst_ref=cards.at[me], send_sem=card_send.at[v], recv_sem=card_recv.at[v],
            device_id={"sub": there}, device_id_type=pl.DeviceIdType.MESH,
        )

    def card_arrival(v):
        return pltpu.make_async_remote_copy(
            src_ref=card, dst_ref=cards.at[(me + n - v) % n], send_sem=card_send.at[v], recv_sem=card_recv.at[v],
            device_id={"sub": (me + n - v) % n}, device_id_type=pl.DeviceIdType.MESH,
        )

    def write_card():
        for load in loads[later + 2 : later + 6]:
            load.wait()
        place = lax.broadcasted_iota(jnp.int32, (half, beams), 0)
        blocks = []
        for child in range(2):
            first = offset_ref[final, 0, child : child + 1, :]
            block = jnp.zeros((half, beams), F32)
            for t in range(taps):
                block = block + jnp.where(place == first + t, weight_ref[final, 0, child, t : t + 1, :], 0.0)
            blocks.append(block)
        eye = lax.broadcasted_iota(jnp.int32, (half, half), 0) == lax.broadcasted_iota(jnp.int32, (half, half), 1)
        for row in (shift_ref[final, 0, 1:2, :].astype(F32), phase_ref[final, 0, 1:2, :]):
            blocks.append(jnp.sum(jnp.where(eye, row, 0.0), axis=1, keepdims=True))
        blocks.append(jnp.zeros((half, LANES - 2 * beams - 2), F32))
        card[...] = jnp.concatenate(blocks, axis=1)

    count = 6 + 2 * taps

    def write_columns():
        raw[...] = jnp.zeros_like(raw)
        for level in range(levels):
            at = level * count
            raw[at : at + 2, :half] = shift_ref[level, 0].astype(F32)
            raw[at + 2 : at + 4, :half] = phase_ref[level, 0]
            raw[at + 4 : at + 6, :beams] = offset_ref[level, 0].astype(F32)
            for child in range(2):
                raw[at + 6 + child * taps : at + 6 + (child + 1) * taps, :beams] = weight_ref[level, 0, child]
        for i in range(raw.shape[0] // LANES):
            columns[i] = raw[i * LANES : (i + 1) * LANES].T

    def prepare(level):
        def column(row, extent):
            at = level * count + row
            return columns[at // LANES, :extent, at % LANES : at % LANES + 1]

        lane = lax.broadcasted_iota(jnp.int32, (beams, LANES), 1)
        shifts = [column(child, half) for child in range(2)]
        phases = [column(2 + child, half) for child in range(2)]
        if level == final:
            card_arrival(n // 2).wait_recv()
            other = cards[(me + n // 2) % n]
            own_first = bit(final) == 0
            a, b = shifts[0], other[:, 2 * beams : 2 * beams + 1]
            shifts = [jnp.where(own_first, a, b), jnp.where(own_first, b, a)]
            a, b = phases[0], other[:, 2 * beams + 1 : 2 * beams + 2]
            phases = [jnp.where(own_first, a, b), jnp.where(own_first, b, a)]
        shift = jnp.concatenate(shifts, axis=0).astype(jnp.int32)
        phase = jnp.concatenate(phases, axis=0)
        signed = jnp.where(lane >= LANES // 2, lane - LANES, lane) * outer
        unit = 2.0 * math.pi / (4 * total)
        coarse = phase - ((signed * shift) & (4 * total - 1)).astype(F32) * unit
        fine = ((lane * shift) & (4 * total - 1)).astype(F32) * (-unit)
        tables[level, 0] = jnp.cos(coarse)
        tables[level, 1] = jnp.sin(coarse)
        tables[level, 2] = jnp.cos(fine)
        tables[level, 3] = jnp.sin(fine)
        if level == final:
            return
        wide = lax.broadcasted_iota(jnp.int32, (beams, extent), 1)
        mask = (
            lax.broadcasted_iota(jnp.int32, (extent, extent), 0) // beams
            == lax.broadcasted_iota(jnp.int32, (extent, extent), 1) // beams
        )
        slot = wide % beams
        second = slot >= half
        place = (slot % half).astype(F32)
        first = jnp.where(second, column(5, beams), column(4, beams))
        block = jnp.zeros((beams, extent), F32)
        for t in range(taps):
            weight = jnp.where(second, column(6 + taps + t, beams), column(6 + t, beams))
            block = block + jnp.where(place == first + t, weight, 0.0)
        tiled = jnp.concatenate([block] * most, axis=0)
        high, low = split(jnp.where(mask, tiled, 0.0))
        merge[level, 0] = high
        merge[level, 1] = low

    def level_copy(level, c):
        return pltpu.make_async_remote_copy(
            src_ref=state.at[level, 1 - bit(level), pl.ds(starts[c], sizes[c])],
            dst_ref=landed.at[level, pl.ds(starts[c], sizes[c])],
            send_sem=level_send.at[level, c],
            recv_sem=level_recv.at[level, c],
            device_id={"sub": across(1 << level)},
            device_id_type=pl.DeviceIdType.MESH,
        )

    def publish(level, c, values):
        values = values.reshape(sizes[c], 2, half, 2 * LANES)
        for h in range(2):
            state[level, h, starts[c] : starts[c] + sizes[c]] = values[:, h]
        level_copy(level, c).start()

    def transformed(values, w_ref):
        high, low = split(values)
        return dot(high, w_ref[0]) + dot(low, w_ref[0]) + dot(high, w_ref[1])

    loads[later + 1].wait()
    for c in range(chunks):
        lines = field[starts[c] : starts[c] + sizes[c]].reshape(sizes[c] * beams, 2 * LANES)
        values = transformed(lines, wf_ref)
        if c == 0:
            pl.semaphore_wait(barrier, n - 1)
        publish(0, c, values)
    write_card()
    for v in range(1, n):
        card_copy(v).start()
    write_columns()
    prepare(0)
    loads[later + 6].wait()

    def turned(level, c, both):
        fr, fi = [], []
        cr, ci = tables[level, 0], tables[level, 1]
        sr, si = tables[level, 2], tables[level, 3]
        for k in range(starts[c], starts[c] + sizes[c]):
            ar, ai = sr[:, k : k + 1], si[:, k : k + 1]
            fr.append(cr * ar - ci * ai)
            fi.append(cr * ai + ci * ar)
        fr, fi = jnp.stack(fr), jnp.stack(fi)
        zr, zi = both[..., :LANES], both[..., LANES:]
        return jnp.concatenate([zr * fr - zi * fi, zr * fi + zi * fr], axis=-1).reshape(sizes[c] * beams, 2 * LANES)

    def stage(level, c):
        level_copy(level, c).wait_recv()
        size, extent = sizes[c], sizes[c] * beams
        at = slice(starts[c], starts[c] + size)
        kept = state[level, bit(level), at]
        both = jnp.concatenate([kept, landed[level, at]], axis=1)
        high, low = split(turned(level, c, both))
        m = [merge[level, i, :extent, :extent] for i in range(2)]
        values = dot(m[0], high) + dot(m[0], low) + dot(m[1], high)
        if level + 1 < final:
            publish(level + 1, c, values)
            return
        values = turned(final, c, values.reshape(size, beams, 2 * LANES))
        back = transformed(values, wi_ref).reshape(size, beams, 2 * LANES)
        for k in range(size):
            at = starts[c] + k
            tr, ti = tw_ref[0, at : at + 1, :], tw_ref[1, at : at + 1, :]
            re, im = back[k, :, :LANES], back[k, :, LANES:]
            field[at, :, :LANES] = re * tr - im * ti
            field[at, :, LANES:] = im * tr + re * ti

    def turn_order(at):
        level, c = at
        return (2.1 * level * outer / 4 + starts[c] if level else c - chunks, level)

    ready = 1
    for level, c in sorted(((a, b) for a in range(final) for b in range(chunks)), key=turn_order):
        while ready <= (final if level == final - 1 else level):
            prepare(ready)
            ready += 1
        stage(level, c)
        if level and ready <= final:
            prepare(ready)
            ready += 1

    for g in range(beams // 8):
        at = slice(g * 8, g * 8 + 8)
        lines = [(field[k, at, :LANES], field[k, at, LANES:]) for k in range(outer)]
        for q, pair in enumerate(butterflies(lines, 1)):
            for p in range(2):
                if groups == 1:
                    sendbuf[q // per, q % per, p, at] = pair[p]
                else:
                    field[q, at, p * LANES : (p + 1) * LANES] = pair[p]
    if groups > 1:
        for q in range(outer):
            for p in range(2):
                line = field[q, :, p * LANES : (p + 1) * LANES]
                for g in range(groups):
                    parts = [line[s * rows : (s + 1) * rows, g * width : (g + 1) * width] for s in range(groups)]
                    sendbuf[q * groups + g, 0, p] = jnp.concatenate(parts, axis=1)

    def turn_copy(v):
        there = (me + v) % n
        return pltpu.make_async_remote_copy(
            src_ref=sendbuf.at[there], dst_ref=gathered.at[me], send_sem=turn_send.at[v], recv_sem=turn_recv.at[v],
            device_id={"sub": there}, device_id_type=pl.DeviceIdType.MESH,
        )

    def turn_arrival(v):
        here = (me + n - v) % n
        return pltpu.make_async_remote_copy(
            src_ref=sendbuf.at[here], dst_ref=gathered.at[here], send_sem=turn_send.at[v], recv_sem=turn_recv.at[v],
            device_id={"sub": here}, device_id_type=pl.DeviceIdType.MESH,
        )

    for v in range(1, n):
        turn_copy(v).start()
    gathered[me] = sendbuf[me]
    cards[me] = card[...]
    for v in range(1, n):
        if v != n // 2:
            card_arrival(v).wait_recv()
    families = n // 16
    if groups == 1:
        lane = lax.broadcasted_iota(jnp.int32, (half, LANES), 1)
        for h in range(2):
            for g in range(families):
                tiles = []
                for side in range(2):
                    for f in range(8):
                        values = cards[h * (n // 2) + g * 8 + f]
                        child = side ^ h
                        moved = pltpu.roll(values, (f - child) * beams % LANES, 1)
                        tiles.append(jnp.where((lane >= f * beams) & (lane < (f + 1) * beams), moved, 0.0))
                high, low = split(jnp.concatenate(tiles, axis=0))
                more[h, g, 0] = high
                more[h, g, 1] = low
    for level in range(final):
        for c in range(chunks):
            level_copy(level, c).wait_send()
    for v in range(1, n):
        card_copy(v).wait_send()
    if groups > 1:
        more[...] = cards[...]
    for v in range(1, n):
        turn_arrival(v).wait_recv()
    for v in range(1, n):
        turn_copy(v).wait_send()


def finish(cfg, gathered, last, out_hbm, out_ref, sem):
    n, per, half = cfg["n"], cfg["per"], cfg["beams"] // 2
    families = n // 16
    stores = []
    for r in range(per):
        for p in range(2):
            for h in range(2):
                for g in range(families):
                    sides = [
                        gathered[at : at + 8, r, p, h * half : (h + 1) * half].reshape(LANES // 2, LANES)
                        for at in (g * 8, n // 2 + g * 8)
                    ]
                    high, low = split(jnp.concatenate(sides, axis=0).T)
                    value = dot(high, last[h, g, 0]) + dot(low, last[h, g, 0]) + dot(high, last[h, g, 1])
                    at = (h * families + g) * LANES
                    out_ref[p, r * LANES : (r + 1) * LANES, at : at + LANES] = value
            at = (p, pl.ds(r * LANES, LANES))
            stores.append(pltpu.make_async_copy(out_ref.at[at], out_hbm.at[at], sem.at[r, p]))
            stores[-1].start()
    for store in stores:
        store.wait()


def real_form(length, direction, factor):
    index = np.arange(length)
    turns = (index[:, None] * index[None, :] % length) * (direction * 2.0 * np.pi / length)
    c, s = np.cos(turns) * factor, np.sin(turns) * factor
    full = np.block([[c, s], [-s, c]]).astype(np.float32)
    high = np.asarray(full, dtype=jnp.bfloat16)
    low = np.asarray(full - high.astype(np.float32), dtype=jnp.bfloat16)
    return np.stack([high, low])


def body(n, sub_images, shift_table, phase_table, offset_table, weight_table):
    beams, bins = sub_images.shape[1], sub_images.shape[2]
    levels, taps = shift_table.shape[0], weight_table.shape[3]
    outer = bins // LANES
    share = bins // n
    per = max(1, share // LANES)
    groups = max(1, LANES // share)
    sizes = tuple(part * outer // sum(CHUNKS) for part in CHUNKS)
    rows = beams // groups
    cfg = dict(n=n, levels=levels, outer=outer, beams=beams, sizes=sizes, per=per, groups=groups,
               width=min(share, LANES), rows=rows, taps=taps)
    turns = np.arange(outer)[:, None] * np.arange(LANES)[None, :] * (2.0 * np.pi / bins)
    twiddle = np.stack([np.cos(turns), np.sin(turns)]).astype(np.float32)
    half = beams // 2
    blocks = -(-levels * (6 + 2 * taps) // LANES)
    shapes = [((n, per, 2, rows, LANES), F32)]
    shapes.append(((2, n // 16, 2, LANES, LANES), BF16) if groups == 1 else ((n, half, LANES), F32))
    held = sum(math.prod(shape) * jnp.dtype(kind).itemsize for shape, kind in shapes)
    vmem = pl.BlockSpec(memory_space=pltpu.VMEM)
    operands = (
        sub_images, shift_table, phase_table, offset_table, weight_table, jnp.asarray(real_form(LANES, -1, 1.0)),
        jnp.asarray(real_form(LANES, 1, 1.0 / bins)), jnp.asarray(twiddle),
    )
    result = pl.pallas_call(
        functools.partial(kernel, cfg),
        name="merges",
        out_shape=[pltpu.VMEM(*shape) for shape in shapes],
        in_specs=[pl.BlockSpec(memory_space=pltpu.HBM)] * 8,
        out_specs=[vmem] * len(shapes),
        scratch_shapes=[
            *[pltpu.VMEM(a.shape, a.dtype) for a in operands],
            pltpu.VMEM((outer, beams, 2 * LANES), F32),
            pltpu.VMEM((levels - 1, 2, outer, half, 2 * LANES), F32),
            pltpu.VMEM((levels - 1, outer, half, 2 * LANES), F32),
            pltpu.VMEM((blocks * LANES, LANES), F32),
            pltpu.VMEM((blocks, LANES, LANES), F32),
            pltpu.VMEM((levels, 4, beams, LANES), F32),
            pltpu.VMEM((levels - 1, 2, max(sizes) * beams, max(sizes) * beams), BF16),
            pltpu.VMEM((n, per, 2, rows, LANES), F32),
            pltpu.VMEM((half, LANES), F32),
            pltpu.VMEM((n, half, LANES), F32),
            pltpu.SemaphoreType.DMA((beams // 8 + 7,)),
            pltpu.SemaphoreType.DMA((levels - 1, len(sizes))),
            pltpu.SemaphoreType.DMA((levels - 1, len(sizes))),
            *[pltpu.SemaphoreType.DMA((n,))] * 4,
        ],
        compiler_params=pltpu.CompilerParams(
            collective_id=0, has_side_effects=True, vmem_limit_bytes=VMEM - held
        ),
    )(*operands)
    if groups == 1:
        shape = (2, per * LANES, n * beams)
        return pl.pallas_call(
            functools.partial(finish, cfg),
            name="finish",
            out_shape=jax.ShapeDtypeStruct(shape, F32),
            in_specs=[vmem] * 2,
            out_specs=pl.BlockSpec(memory_space=pltpu.HBM),
            scratch_shapes=[pltpu.VMEM(shape, F32), pltpu.SemaphoreType.DMA((per, 2))],
            compiler_params=pltpu.CompilerParams(vmem_limit_bytes=24000000),
        )(*result)
    pieces = result[0].reshape(n, 2, rows, groups, share).transpose(1, 4, 0, 3, 2)
    pieces = pieces.reshape(2, share, 2, n // 2, 2, half)
    blocks = result[1][:, :, : 2 * beams].reshape(2, n // 2, half, 2, beams)
    sums = []
    for h in range(2):
        total = 0.0
        for child in range(2):
            total = total + jnp.einsum(
                "pqim,imj->pqij", pieces[:, :, h ^ child, :, h], blocks[h, :, :, child], precision=lax.Precision.HIGHEST
            )
        sums.append(total)
    return jnp.stack(sums, axis=2).reshape(2, share, n * beams)


def solution(mesh):
    placed = (
        P(None, ("img", "sub"), None),
        P(None, "sub", None, None),
        P(None, "sub", None, None),
        P(None, "sub", None, None),
        P(None, "sub", None, None, None),
    )
    return jax.shard_map(
        functools.partial(body, mesh.shape["sub"]),
        mesh=mesh, in_specs=placed, out_specs=P(None, ("img", "sub"), None), check_vma=False,
    )
```

```python
import functools
import math

import jax
import jax.numpy as jnp
import numpy as np
from jax import lax
from jax.experimental import pallas as pl
from jax.experimental.pallas import tpu as pltpu
from jax.sharding import PartitionSpec as P

LANES = 128
CHUNKS = (1, 1, 2, 2, 1, 1)
VMEM = 67043328 - (3 << 16)
F32 = jnp.float32
BF16 = jnp.bfloat16


def split(values):
    high = values.astype(BF16)
    low = (values - high.astype(F32)).astype(BF16)
    return high, low


def dot(left, right):
    return jnp.dot(left, right, preferred_element_type=F32)


def times_constant(pair, constant):
    real_part, imag_part = pair
    c, s = constant.real, constant.imag
    if abs(s) < 1e-12:
        return pair if c > 0 else (-real_part, -imag_part)
    if abs(c) < 1e-12:
        return (-imag_part, real_part) if s > 0 else (imag_part, -real_part)
    if abs(abs(c) - abs(s)) < 1e-12:
        h = abs(c)
        a = real_part if c > 0 else -real_part
        b = imag_part if s > 0 else -imag_part
        e = real_part if s > 0 else -real_part
        f = imag_part if c > 0 else -imag_part
        return (a - b) * h, (e + f) * h
    return real_part * c - imag_part * s, real_part * s + imag_part * c


def butterflies(rows, direction):
    n = len(rows)
    if n == 1:
        return rows
    even = butterflies(rows[0::2], direction)
    odd = butterflies(rows[1::2], direction)
    first, second = [], []
    for k in range(n // 2):
        angle = direction * 2.0 * math.pi * k / n
        tr, ti = times_constant(odd[k], complex(math.cos(angle), math.sin(angle)))
        er, ei = even[k]
        first.append((er + tr, ei + ti))
        second.append((er - tr, ei - ti))
    return first + second


def kernel(cfg, x_hbm, shift_hbm, phase_hbm, offset_hbm, weight_hbm, wf_hbm, wi_hbm, tw_hbm, *refs):
    gathered, more, refs = refs[0], refs[1], refs[2:]
    (x_ref, shift_ref, phase_ref, offset_ref, weight_ref, wf_ref, wi_ref, tw_ref,
     field, state, landed, raw, columns, tables, merge, sendbuf, card, cards, extra, packed,
     load_sem, level_send, level_recv, turn_send, turn_recv, card_send, card_recv,
     extra_send, extra_recv, share_send, share_recv) = refs
    n, levels, outer, beams, sizes = cfg["n"], cfg["levels"], cfg["outer"], cfg["beams"], cfg["sizes"]
    per, groups, width, rows = cfg["per"], cfg["groups"], cfg["width"], cfg["rows"]
    half = beams // 2
    chunks = len(sizes)
    starts = [sum(sizes[:c]) for c in range(chunks)]
    most = max(sizes)
    extent = most * beams
    taps = cfg["taps"]
    total = outer * LANES
    final = levels - 1
    me = lax.axis_index("sub")

    twice = cfg["twice"]

    def bit_of(device, level):
        return (device // (1 << level)) % 2

    def bit(level):
        return bit_of(me, level)

    def inner(device):
        return (bit_of(device, final) + bit_of(device, final - 1)) % 2 * bit_of(device, 0)

    def facing(device):
        for level in (final - 1, final):
            device = device + (1 - 2 * bit_of(device, level)) * (1 << level)
        return device

    def partial(source, target):
        return inner(source) * ((bit_of(source, final) + bit_of(target, final)) % 2)

    def across(mask):
        other = me
        for level in range(levels):
            if mask >> level & 1:
                other = other + (1 - 2 * bit(level)) * (1 << level)
        return other

    pairs = [(x_hbm.at[:, pl.ds(g * 8, 8)], x_ref.at[:, pl.ds(g * 8, 8)]) for g in range(beams // 8)]
    pairs += [(tw_hbm, tw_ref), (wf_hbm, wf_ref), (shift_hbm, shift_ref), (phase_hbm, phase_ref),
              (offset_hbm, offset_ref), (weight_hbm, weight_ref), (wi_hbm, wi_ref)]
    loads = [pltpu.make_async_copy(src, dst, load_sem.at[i]) for i, (src, dst) in enumerate(pairs)]
    for load in loads:
        load.start()

    barrier = pltpu.get_barrier_semaphore()
    for mask in range(1, n):
        pl.semaphore_signal(barrier, inc=1, device_id={"sub": across(mask)}, device_id_type=pl.DeviceIdType.MESH)

    later = beams // 8
    for g in range(beams // 8):
        loads[g].wait()
        if g == 0:
            loads[later].wait()
        lines = [
            tuple(x_ref[p, g * 8 : g * 8 + 8, q * LANES : (q + 1) * LANES] for p in range(2)) for q in range(outer)
        ]
        for k, (re, im) in enumerate(butterflies(lines, -1)):
            tr, ti = tw_ref[0, k : k + 1, :], tw_ref[1, k : k + 1, :]
            field[k, g * 8 : g * 8 + 8, :LANES] = re * tr + im * ti
            field[k, g * 8 : g * 8 + 8, LANES:] = im * tr - re * ti

    def card_copy(v):
        there = (me + v) % n
        return pltpu.make_async_remote_copy(
            src_ref=card, dst_ref=cards.at[me], send_sem=card_send.at[v], recv_sem=card_recv.at[v],
            device_id={"sub": there}, device_id_type=pl.DeviceIdType.MESH,
        )

    def card_arrival(v):
        return pltpu.make_async_remote_copy(
            src_ref=card, dst_ref=cards.at[(me + n - v) % n], send_sem=card_send.at[v], recv_sem=card_recv.at[v],
            device_id={"sub": (me + n - v) % n}, device_id_type=pl.DeviceIdType.MESH,
        )

    def write_card():
        for load in loads[later + 2 : later + 6]:
            load.wait()
        place = lax.broadcasted_iota(jnp.int32, (half, beams), 0)
        blocks = []
        for child in range(2):
            first = offset_ref[final, 0, child : child + 1, :]
            block = jnp.zeros((half, beams), F32)
            for t in range(taps):
                block = block + jnp.where(place == first + t, weight_ref[final, 0, child, t : t + 1, :], 0.0)
            blocks.append(block)
        eye = lax.broadcasted_iota(jnp.int32, (half, half), 0) == lax.broadcasted_iota(jnp.int32, (half, half), 1)
        for row in (shift_ref[final, 0, 1:2, :].astype(F32), phase_ref[final, 0, 1:2, :]):
            blocks.append(jnp.sum(jnp.where(eye, row, 0.0), axis=1, keepdims=True))
        blocks.append(jnp.zeros((half, LANES - 2 * beams - 2), F32))
        card[...] = jnp.concatenate(blocks, axis=1)

    count = 6 + 2 * taps

    def write_columns():
        raw[...] = jnp.zeros_like(raw)
        for level in range(levels):
            at = level * count
            raw[at : at + 2, :half] = shift_ref[level, 0].astype(F32)
            raw[at + 2 : at + 4, :half] = phase_ref[level, 0]
            raw[at + 4 : at + 6, :beams] = offset_ref[level, 0].astype(F32)
            for child in range(2):
                raw[at + 6 + child * taps : at + 6 + (child + 1) * taps, :beams] = weight_ref[level, 0, child]
        for i in range(raw.shape[0] // LANES):
            columns[i] = raw[i * LANES : (i + 1) * LANES].T

    def prepare(level):
        def column(row, extent):
            at = level * count + row
            return columns[at // LANES, :extent, at % LANES : at % LANES + 1]

        lane = lax.broadcasted_iota(jnp.int32, (beams, LANES), 1)
        shifts = [column(child, half) for child in range(2)]
        phases = [column(2 + child, half) for child in range(2)]
        if level == final:
            card_arrival(n // 2).wait_recv()
            other = cards[(me + n // 2) % n]
            own_first = bit(final) == 0
            a, b = shifts[0], other[:, 2 * beams : 2 * beams + 1]
            shifts = [jnp.where(own_first, a, b), jnp.where(own_first, b, a)]
            a, b = phases[0], other[:, 2 * beams + 1 : 2 * beams + 2]
            phases = [jnp.where(own_first, a, b), jnp.where(own_first, b, a)]
        shift = jnp.concatenate(shifts, axis=0).astype(jnp.int32)
        phase = jnp.concatenate(phases, axis=0)
        signed = jnp.where(lane >= LANES // 2, lane - LANES, lane) * outer
        unit = 2.0 * math.pi / (4 * total)
        coarse = phase - ((signed * shift) & (4 * total - 1)).astype(F32) * unit
        fine = ((lane * shift) & (4 * total - 1)).astype(F32) * (-unit)
        tables[level, 0] = jnp.cos(coarse)
        tables[level, 1] = jnp.sin(coarse)
        tables[level, 2] = jnp.cos(fine)
        tables[level, 3] = jnp.sin(fine)
        if level == final:
            return
        wide = lax.broadcasted_iota(jnp.int32, (beams, extent), 1)
        mask = (
            lax.broadcasted_iota(jnp.int32, (extent, extent), 0) // beams
            == lax.broadcasted_iota(jnp.int32, (extent, extent), 1) // beams
        )
        slot = wide % beams
        second = slot >= half
        place = (slot % half).astype(F32)
        first = jnp.where(second, column(5, beams), column(4, beams))
        block = jnp.zeros((beams, extent), F32)
        for t in range(taps):
            weight = jnp.where(second, column(6 + taps + t, beams), column(6 + t, beams))
            block = block + jnp.where(place == first + t, weight, 0.0)
        tiled = jnp.concatenate([block] * most, axis=0)
        high, low = split(jnp.where(mask, tiled, 0.0))
        merge[level, 0] = high
        merge[level, 1] = low

    def level_copy(level, c):
        return pltpu.make_async_remote_copy(
            src_ref=state.at[level, 1 - bit(level), pl.ds(starts[c], sizes[c])],
            dst_ref=landed.at[level, pl.ds(starts[c], sizes[c])],
            send_sem=level_send.at[level, c],
            recv_sem=level_recv.at[level, c],
            device_id={"sub": across(1 << level)},
            device_id_type=pl.DeviceIdType.MESH,
        )

    def publish(level, c, values):
        values = values.reshape(sizes[c], 2, half, 2 * LANES)
        for h in range(2):
            state[level, h, starts[c] : starts[c] + sizes[c]] = values[:, h]
        level_copy(level, c).start()

    def transformed(values, w_ref):
        high, low = split(values)
        return dot(high, w_ref[0]) + dot(low, w_ref[0]) + dot(high, w_ref[1])

    loads[later + 1].wait()
    for c in range(chunks):
        lines = field[starts[c] : starts[c] + sizes[c]].reshape(sizes[c] * beams, 2 * LANES)
        values = transformed(lines, wf_ref)
        if c == 0:
            pl.semaphore_wait(barrier, n - 1)
        publish(0, c, values)
    write_card()
    for v in range(1, n):
        card_copy(v).start()
    write_columns()
    prepare(0)
    loads[later + 6].wait()

    def turned(level, c, both):
        fr, fi = [], []
        cr, ci = tables[level, 0], tables[level, 1]
        sr, si = tables[level, 2], tables[level, 3]
        for k in range(starts[c], starts[c] + sizes[c]):
            ar, ai = sr[:, k : k + 1], si[:, k : k + 1]
            fr.append(cr * ar - ci * ai)
            fi.append(cr * ai + ci * ar)
        fr, fi = jnp.stack(fr), jnp.stack(fi)
        zr, zi = both[..., :LANES], both[..., LANES:]
        return jnp.concatenate([zr * fr - zi * fi, zr * fi + zi * fr], axis=-1).reshape(sizes[c] * beams, 2 * LANES)

    def stage(level, c):
        level_copy(level, c).wait_recv()
        size, extent = sizes[c], sizes[c] * beams
        at = slice(starts[c], starts[c] + size)
        kept = state[level, bit(level), at]
        both = jnp.concatenate([kept, landed[level, at]], axis=1)
        high, low = split(turned(level, c, both))
        m = [merge[level, i, :extent, :extent] for i in range(2)]
        values = dot(m[0], high) + dot(m[0], low) + dot(m[1], high)
        if level + 1 < final:
            publish(level + 1, c, values)
            return
        values = turned(final, c, values.reshape(size, beams, 2 * LANES))
        back = transformed(values, wi_ref).reshape(size, beams, 2 * LANES)
        for k in range(size):
            at = starts[c] + k
            tr, ti = tw_ref[0, at : at + 1, :], tw_ref[1, at : at + 1, :]
            re, im = back[k, :, :LANES], back[k, :, LANES:]
            field[at, :, :LANES] = re * tr - im * ti
            field[at, :, LANES:] = im * tr + re * ti
        if twice:

            @pl.when(inner(me) == 1)
            def _():
                extra_copy(c).start()

    def extra_copy(c):
        at = pl.ds(starts[c], sizes[c])
        return pltpu.make_async_remote_copy(
            src_ref=field.at[at, pl.ds(half, half)], dst_ref=extra.at[at],
            send_sem=extra_send.at[c], recv_sem=extra_recv.at[c],
            device_id={"sub": facing(me)}, device_id_type=pl.DeviceIdType.MESH,
        )

    def turn_order(at):
        level, c = at
        return (20 * level * outer / 32 + starts[c] if level else c - chunks, level)

    ready = 1
    for level, c in sorted(((a, b) for a in range(final) for b in range(chunks)), key=turn_order):
        while ready <= (final if level == final - 1 else level):
            prepare(ready)
            ready += 1
        stage(level, c)
        if level and ready <= final:
            prepare(ready)
            ready += 1

    for g in range(beams // 8):
        at = slice(g * 8, g * 8 + 8)
        lines = [(field[k, at, :LANES], field[k, at, LANES:]) for k in range(outer)]
        for q, pair in enumerate(butterflies(lines, 1)):
            for p in range(2):
                if groups == 1:
                    sendbuf[q // per, q % per, p, at] = pair[p]
                else:
                    field[q, at, p * LANES : (p + 1) * LANES] = pair[p]
    if groups > 1:
        for q in range(outer):
            for p in range(2):
                line = field[q, :, p * LANES : (p + 1) * LANES]
                for g in range(groups):
                    parts = [line[s * rows : (s + 1) * rows, g * width : (g + 1) * width] for s in range(groups)]
                    sendbuf[q * groups + g, 0, p] = jnp.concatenate(parts, axis=1)

    def turn_copy(v, source, lines):
        target = (source + v) % n
        here = target if source is me else source
        return pltpu.make_async_remote_copy(
            src_ref=sendbuf.at[here, :, :, pl.ds(0, lines)], dst_ref=gathered.at[source, :, :, pl.ds(0, lines)],
            send_sem=turn_send.at[v], recv_sem=turn_recv.at[v],
            device_id={"sub": here}, device_id_type=pl.DeviceIdType.MESH,
        )

    def each_turn(v, arrives, act):
        source = (me + n - v) % n if arrives else me
        if not twice:
            act(turn_copy(v, source, rows))
            return
        part = partial(source, (source + v) % n)

        @pl.when(part == 0)
        def _():
            act(turn_copy(v, source, rows))

        @pl.when(part == 1)
        def _():
            act(turn_copy(v, source, half))

    def share_copy(slot, source, target):
        return pltpu.make_async_remote_copy(
            src_ref=packed.at[slot], dst_ref=gathered.at[facing(source), :, :, pl.ds(half, half)],
            send_sem=share_send.at[slot], recv_sem=share_recv.at[source % (n // 2)],
            device_id={"sub": target}, device_id_type=pl.DeviceIdType.MESH,
        )

    def each_share(act):
        for slot in range(n // 2):
            target = bit(final) * (n // 2) + slot

            @pl.when(inner(me) * jnp.where(target == me, 0, 1) == 1)
            def _():
                act(share_copy(slot, me, target))

    for v in range(1, n):
        each_turn(v, False, lambda copy: copy.start())
    if twice:

        @pl.when(inner(me) == 1)
        def _():
            for c in range(chunks):
                extra_copy(c).wait_recv()
            lines = [(extra[k, :, :LANES], extra[k, :, LANES:]) for k in range(outer)]
            even, odd = butterflies(lines[0::2], 1), butterflies(lines[1::2], 1)
            sign = (1 - 2 * bit(final)).astype(F32)
            for k in range(outer // 2):
                angle = 2.0 * math.pi * k / outer
                turn = times_constant(odd[k], complex(math.cos(angle), math.sin(angle)))
                for p in range(2):
                    packed[k // per, k % per, p] = even[k][p] + sign * turn[p]

        each_share(lambda copy: copy.start())

        @pl.when(inner(me) == 1)
        def _():
            gathered[facing(me), :, :, half:] = packed[me % (n // 2)]

    gathered[me] = sendbuf[me]
    cards[me] = card[...]
    for v in range(1, n):
        if v != n // 2:
            card_arrival(v).wait_recv()
    families = n // 16
    if groups == 1:
        lane = lax.broadcasted_iota(jnp.int32, (half, LANES), 1)
        for h in range(2):
            for g in range(families):
                tiles = []
                for side in range(2):
                    for f in range(8):
                        values = cards[h * (n // 2) + g * 8 + f]
                        child = side ^ h
                        moved = pltpu.roll(values, (f - child) * beams % LANES, 1)
                        tiles.append(jnp.where((lane >= f * beams) & (lane < (f + 1) * beams), moved, 0.0))
                high, low = split(jnp.concatenate(tiles, axis=0))
                more[h, g, 0] = high
                more[h, g, 1] = low
    for level in range(final):
        for c in range(chunks):
            level_copy(level, c).wait_send()
    for v in range(1, n):
        card_copy(v).wait_send()
    if groups > 1:
        more[...] = cards[...]
    for v in range(1, n):
        each_turn(v, True, lambda copy: copy.wait_recv())
    if twice:
        for slot in range(n // 2):
            source = bit(final) * (n // 2) + slot

            @pl.when(inner(source) * jnp.where(source == me, 0, 1) == 1)
            def _():
                share_copy(slot, source, source).wait_recv()
    for v in range(1, n):
        each_turn(v, False, lambda copy: copy.wait_send())
    if twice:
        each_share(lambda copy: copy.wait_send())

        @pl.when(inner(me) == 1)
        def _():
            for c in range(chunks):
                extra_copy(c).wait_send()


def finish(cfg, gathered, last, out_hbm, out_ref, sem):
    n, per, half = cfg["n"], cfg["per"], cfg["beams"] // 2
    families = n // 16
    stores = []
    for r in range(per):
        for p in range(2):
            for h in range(2):
                for g in range(families):
                    sides = [
                        gathered[at : at + 8, r, p, h * half : (h + 1) * half].reshape(LANES // 2, LANES)
                        for at in (g * 8, n // 2 + g * 8)
                    ]
                    high, low = split(jnp.concatenate(sides, axis=0).T)
                    value = dot(high, last[h, g, 0]) + dot(low, last[h, g, 0]) + dot(high, last[h, g, 1])
                    at = (h * families + g) * LANES
                    out_ref[p, r * LANES : (r + 1) * LANES, at : at + LANES] = value
            at = (p, pl.ds(r * LANES, LANES))
            stores.append(pltpu.make_async_copy(out_ref.at[at], out_hbm.at[at], sem.at[r, p]))
            stores[-1].start()
    for store in stores:
        store.wait()


def real_form(length, direction, factor):
    index = np.arange(length)
    turns = (index[:, None] * index[None, :] % length) * (direction * 2.0 * np.pi / length)
    c, s = np.cos(turns) * factor, np.sin(turns) * factor
    full = np.block([[c, s], [-s, c]]).astype(np.float32)
    high = np.asarray(full, dtype=jnp.bfloat16)
    low = np.asarray(full - high.astype(np.float32), dtype=jnp.bfloat16)
    return np.stack([high, low])


def body(n, sub_images, shift_table, phase_table, offset_table, weight_table):
    beams, bins = sub_images.shape[1], sub_images.shape[2]
    levels, taps = shift_table.shape[0], weight_table.shape[3]
    outer = bins // LANES
    share = bins // n
    per = max(1, share // LANES)
    groups = max(1, LANES // share)
    sizes = tuple(part * outer // sum(CHUNKS) for part in CHUNKS)
    rows = beams // groups
    cfg = dict(n=n, levels=levels, outer=outer, beams=beams, sizes=sizes, per=per, groups=groups,
               width=min(share, LANES), rows=rows, taps=taps, twice=groups == 1 and levels > 2)
    turns = np.arange(outer)[:, None] * np.arange(LANES)[None, :] * (2.0 * np.pi / bins)
    twiddle = np.stack([np.cos(turns), np.sin(turns)]).astype(np.float32)
    half = beams // 2
    blocks = -(-levels * (6 + 2 * taps) // LANES)
    shapes = [((n, per, 2, rows, LANES), F32)]
    shapes.append(((2, n // 16, 2, LANES, LANES), BF16) if groups == 1 else ((n, half, LANES), F32))
    held = sum(math.prod(shape) * jnp.dtype(kind).itemsize for shape, kind in shapes)
    vmem = pl.BlockSpec(memory_space=pltpu.VMEM)
    operands = (
        sub_images, shift_table, phase_table, offset_table, weight_table, jnp.asarray(real_form(LANES, -1, 1.0)),
        jnp.asarray(real_form(LANES, 1, 1.0 / bins)), jnp.asarray(twiddle),
    )
    result = pl.pallas_call(
        functools.partial(kernel, cfg),
        name="merges",
        out_shape=[pltpu.VMEM(*shape) for shape in shapes],
        in_specs=[pl.BlockSpec(memory_space=pltpu.HBM)] * 8,
        out_specs=[vmem] * len(shapes),
        scratch_shapes=[
            *[pltpu.VMEM(a.shape, a.dtype) for a in operands],
            pltpu.VMEM((outer, beams, 2 * LANES), F32),
            pltpu.VMEM((levels - 1, 2, outer, half, 2 * LANES), F32),
            pltpu.VMEM((levels - 1, outer, half, 2 * LANES), F32),
            pltpu.VMEM((blocks * LANES, LANES), F32),
            pltpu.VMEM((blocks, LANES, LANES), F32),
            pltpu.VMEM((levels, 4, beams, LANES), F32),
            pltpu.VMEM((levels - 1, 2, max(sizes) * beams, max(sizes) * beams), BF16),
            pltpu.VMEM((n, per, 2, rows, LANES), F32),
            pltpu.VMEM((half, LANES), F32),
            pltpu.VMEM((n, half, LANES), F32),
            pltpu.VMEM((outer, half, 2 * LANES), F32),
            pltpu.VMEM((n // 2, per, 2, half, LANES), F32),
            pltpu.SemaphoreType.DMA((beams // 8 + 7,)),
            pltpu.SemaphoreType.DMA((levels - 1, len(sizes))),
            pltpu.SemaphoreType.DMA((levels - 1, len(sizes))),
            *[pltpu.SemaphoreType.DMA((n,))] * 4,
            *[pltpu.SemaphoreType.DMA((len(sizes),))] * 2,
            *[pltpu.SemaphoreType.DMA((n // 2,))] * 2,
        ],
        compiler_params=pltpu.CompilerParams(
            collective_id=0, has_side_effects=True, vmem_limit_bytes=VMEM - held
        ),
    )(*operands)
    if groups == 1:
        shape = (2, per * LANES, n * beams)
        return pl.pallas_call(
            functools.partial(finish, cfg),
            name="finish",
            out_shape=jax.ShapeDtypeStruct(shape, F32),
            in_specs=[vmem] * 2,
            out_specs=pl.BlockSpec(memory_space=pltpu.HBM),
            scratch_shapes=[pltpu.VMEM(shape, F32), pltpu.SemaphoreType.DMA((per, 2))],
            compiler_params=pltpu.CompilerParams(vmem_limit_bytes=24000000),
        )(*result)
    pieces = result[0].reshape(n, 2, rows, groups, share).transpose(1, 4, 0, 3, 2)
    pieces = pieces.reshape(2, share, 2, n // 2, 2, half)
    blocks = result[1][:, :, : 2 * beams].reshape(2, n // 2, half, 2, beams)
    sums = []
    for h in range(2):
        total = 0.0
        for child in range(2):
            total = total + jnp.einsum(
                "pqim,imj->pqij", pieces[:, :, h ^ child, :, h], blocks[h, :, :, child], precision=lax.Precision.HIGHEST
            )
        sums.append(total)
    return jnp.stack(sums, axis=2).reshape(2, share, n * beams)


def solution(mesh):
    placed = (
        P(None, ("img", "sub"), None),
        P(None, "sub", None, None),
        P(None, "sub", None, None),
        P(None, "sub", None, None),
        P(None, "sub", None, None, None),
    )
    return jax.shard_map(
        functools.partial(body, mesh.shape["sub"]),
        mesh=mesh, in_specs=placed, out_specs=P(None, ("img", "sub"), None), check_vma=False,
    )
```

```python
import functools
import math

import jax
import jax.numpy as jnp
import numpy as np
from jax import lax
from jax.experimental import pallas as pl
from jax.experimental.pallas import tpu as pltpu
from jax.sharding import PartitionSpec as P

LANES = 128
CHUNKS = (1, 2, 2, 1, 1, 1)
AHEAD = 3
GAP = 20
VMEM = 67043328 - (3 << 16)
F32 = jnp.float32
BF16 = jnp.bfloat16


def split(values):
    high = values.astype(BF16)
    low = (values - high.astype(F32)).astype(BF16)
    return high, low


def dot(left, right):
    return jnp.dot(left, right, preferred_element_type=F32)


def times_constant(pair, constant):
    real_part, imag_part = pair
    c, s = constant.real, constant.imag
    if abs(s) < 1e-12:
        return pair if c > 0 else (-real_part, -imag_part)
    if abs(c) < 1e-12:
        return (-imag_part, real_part) if s > 0 else (imag_part, -real_part)
    if abs(abs(c) - abs(s)) < 1e-12:
        h = abs(c)
        a = real_part if c > 0 else -real_part
        b = imag_part if s > 0 else -imag_part
        e = real_part if s > 0 else -real_part
        f = imag_part if c > 0 else -imag_part
        return (a - b) * h, (e + f) * h
    return real_part * c - imag_part * s, real_part * s + imag_part * c


def butterflies(rows, direction):
    n = len(rows)
    if n == 1:
        return rows
    even = butterflies(rows[0::2], direction)
    odd = butterflies(rows[1::2], direction)
    first, second = [], []
    for k in range(n // 2):
        angle = direction * 2.0 * math.pi * k / n
        tr, ti = times_constant(odd[k], complex(math.cos(angle), math.sin(angle)))
        er, ei = even[k]
        first.append((er + tr, ei + ti))
        second.append((er - tr, ei - ti))
    return first + second


def kernel(cfg, x_hbm, shift_hbm, phase_hbm, offset_hbm, weight_hbm, wf_hbm, wi_hbm, tw_hbm, *refs):
    gathered, more, refs = refs[0], refs[1], refs[2:]
    (x_ref, shift_ref, phase_ref, offset_ref, weight_ref, wf_ref, wi_ref, tw_ref,
     field, state, landed, raw, columns, tables, merge, sendbuf, card, cards, extra, packed,
     load_sem, level_send, level_recv, pooled) = refs
    turn_send, turn_recv, card_send, card_recv, facing_recv, extra_send, extra_recv, share_send, share_recv = (
        pooled.at[i] for i in range(9)
    )
    n, levels, outer, beams, sizes = cfg["n"], cfg["levels"], cfg["outer"], cfg["beams"], cfg["sizes"]
    per, groups, width, rows = cfg["per"], cfg["groups"], cfg["width"], cfg["rows"]
    half = beams // 2
    chunks = len(sizes)
    starts = [sum(sizes[:c]) for c in range(chunks)]
    most = max(sizes)
    extent = most * beams
    taps = cfg["taps"]
    total = outer * LANES
    final = levels - 1
    me = lax.axis_index("sub")

    twice = cfg["twice"]

    def bit_of(device, level):
        return (device // (1 << level)) % 2

    def bit(level):
        return bit_of(me, level)

    def inner(device):
        return (bit_of(device, final) + bit_of(device, final - 1)) % 2 * bit_of(device, 0)

    def facing(device):
        for level in (final - 1, final):
            device = device + (1 - 2 * bit_of(device, level)) * (1 << level)
        return device

    def across(mask):
        other = me
        for level in range(levels):
            if mask >> level & 1:
                other = other + (1 - 2 * bit(level)) * (1 << level)
        return other

    pairs = [(x_hbm.at[:, pl.ds(g * 8, 8)], x_ref.at[:, pl.ds(g * 8, 8)]) for g in range(beams // 8)]
    pairs += [(tw_hbm, tw_ref), (wf_hbm, wf_ref), (shift_hbm, shift_ref), (phase_hbm, phase_ref),
              (offset_hbm, offset_ref), (weight_hbm, weight_ref), (wi_hbm, wi_ref)]
    loads = [pltpu.make_async_copy(src, dst, load_sem.at[i]) for i, (src, dst) in enumerate(pairs)]
    for load in loads:
        load.start()

    barrier = pltpu.get_barrier_semaphore()
    for mask in range(1, n):
        pl.semaphore_signal(barrier, inc=1, device_id={"sub": across(mask)}, device_id_type=pl.DeviceIdType.MESH)

    later = beams // 8
    for g in range(beams // 8):
        loads[g].wait()
        if g == 0:
            loads[later].wait()
        lines = [
            tuple(x_ref[p, g * 8 : g * 8 + 8, q * LANES : (q + 1) * LANES] for p in range(2)) for q in range(outer)
        ]
        for k, (re, im) in enumerate(butterflies(lines, -1)):
            tr, ti = tw_ref[0, k : k + 1, :], tw_ref[1, k : k + 1, :]
            field[k, g * 8 : g * 8 + 8, :LANES] = re * tr + im * ti
            field[k, g * 8 : g * 8 + 8, LANES:] = im * tr - re * ti

    def all_of(source, target, send, recv):
        return pltpu.make_async_remote_copy(
            src_ref=source, dst_ref=target, send_sem=send, recv_sem=recv,
            device_id={"sub": across(1)}, device_id_type=pl.DeviceIdType.MESH,
        )

    def card_copy(v):
        there = (me + v) % n
        return pltpu.make_async_remote_copy(
            src_ref=card, dst_ref=cards.at[me], send_sem=card_send, recv_sem=facing_recv if v == n // 2 else card_recv,
            device_id={"sub": there}, device_id_type=pl.DeviceIdType.MESH,
        )

    def write_card():
        place = lax.broadcasted_iota(jnp.int32, (half, beams), 0)
        blocks = []
        for child in range(2):
            first = offset_ref[final, 0, child : child + 1, :]
            block = jnp.zeros((half, beams), F32)
            for t in range(taps):
                block = block + jnp.where(place == first + t, weight_ref[final, 0, child, t : t + 1, :], 0.0)
            blocks.append(block)
        eye = lax.broadcasted_iota(jnp.int32, (half, half), 0) == lax.broadcasted_iota(jnp.int32, (half, half), 1)
        for row in (shift_ref[final, 0, 1:2, :].astype(F32), phase_ref[final, 0, 1:2, :]):
            blocks.append(jnp.sum(jnp.where(eye, row, 0.0), axis=1, keepdims=True))
        blocks.append(jnp.zeros((half, LANES - 2 * beams - 2), F32))
        card[...] = jnp.concatenate(blocks, axis=1)

    count = 6 + 2 * taps

    def write_columns():
        raw[...] = jnp.zeros_like(raw)
        for level in range(levels):
            at = level * count
            raw[at : at + 2, :half] = shift_ref[level, 0].astype(F32)
            raw[at + 2 : at + 4, :half] = phase_ref[level, 0]
            raw[at + 4 : at + 6, :beams] = offset_ref[level, 0].astype(F32)
            for child in range(2):
                raw[at + 6 + child * taps : at + 6 + (child + 1) * taps, :beams] = weight_ref[level, 0, child]
        for i in range(raw.shape[0] // LANES):
            columns[i] = raw[i * LANES : (i + 1) * LANES].T

    def prepare(level):
        def column(row, extent):
            at = level * count + row
            return columns[at // LANES, :extent, at % LANES : at % LANES + 1]

        lane = lax.broadcasted_iota(jnp.int32, (beams, LANES), 1)
        shifts = [column(child, half) for child in range(2)]
        phases = [column(2 + child, half) for child in range(2)]
        if level == final:
            opposite = (me + n // 2) % n
            all_of(card, cards.at[opposite], card_send, facing_recv).wait_recv()
            other = cards[opposite]
            own_first = bit(final) == 0
            a, b = shifts[0], other[:, 2 * beams : 2 * beams + 1]
            shifts = [jnp.where(own_first, a, b), jnp.where(own_first, b, a)]
            a, b = phases[0], other[:, 2 * beams + 1 : 2 * beams + 2]
            phases = [jnp.where(own_first, a, b), jnp.where(own_first, b, a)]
        shift = jnp.concatenate(shifts, axis=0).astype(jnp.int32)
        phase = jnp.concatenate(phases, axis=0)
        signed = jnp.where(lane >= LANES // 2, lane - LANES, lane) * outer
        unit = 2.0 * math.pi / (4 * total)
        coarse = phase - ((signed * shift) & (4 * total - 1)).astype(F32) * unit
        fine = ((lane * shift) & (4 * total - 1)).astype(F32) * (-unit)
        tables[level, 0] = jnp.cos(coarse)
        tables[level, 1] = jnp.sin(coarse)
        tables[level, 2] = jnp.cos(fine)
        tables[level, 3] = jnp.sin(fine)
        if level == final:
            return
        wide = lax.broadcasted_iota(jnp.int32, (beams, extent), 1)
        mask = (
            lax.broadcasted_iota(jnp.int32, (extent, extent), 0) // beams
            == lax.broadcasted_iota(jnp.int32, (extent, extent), 1) // beams
        )
        slot = wide % beams
        second = slot >= half
        place = (slot % half).astype(F32)
        first = jnp.where(second, column(5, beams), column(4, beams))
        block = jnp.zeros((beams, extent), F32)
        for t in range(taps):
            weight = jnp.where(second, column(6 + taps + t, beams), column(6 + t, beams))
            block = block + jnp.where(place == first + t, weight, 0.0)
        tiled = jnp.concatenate([block] * most, axis=0)
        high, low = split(jnp.where(mask, tiled, 0.0))
        merge[level, 0] = high
        merge[level, 1] = low

    def level_copy(level, c):
        return pltpu.make_async_remote_copy(
            src_ref=state.at[level, 1 - bit(level), pl.ds(starts[c], sizes[c])],
            dst_ref=landed.at[level, pl.ds(starts[c], sizes[c])],
            send_sem=level_send.at[level],
            recv_sem=level_recv.at[level, c],
            device_id={"sub": across(1 << level)},
            device_id_type=pl.DeviceIdType.MESH,
        )

    def publish(level, c, values):
        values = values.reshape(sizes[c], 2, half, 2 * LANES)
        for h in range(2):
            state[level, h, starts[c] : starts[c] + sizes[c]] = values[:, h]
        level_copy(level, c).start()

    def transformed(values, w_ref):
        high, low = split(values)
        return dot(high, w_ref[0]) + dot(low, w_ref[0]) + dot(high, w_ref[1])

    def turned(level, c, both):
        fr, fi = [], []
        cr, ci = tables[level, 0], tables[level, 1]
        sr, si = tables[level, 2], tables[level, 3]
        for k in range(starts[c], starts[c] + sizes[c]):
            ar, ai = sr[:, k : k + 1], si[:, k : k + 1]
            fr.append(cr * ar - ci * ai)
            fi.append(cr * ai + ci * ar)
        fr, fi = jnp.stack(fr), jnp.stack(fi)
        zr, zi = both[..., :LANES], both[..., LANES:]
        return jnp.concatenate([zr * fr - zi * fi, zr * fi + zi * fr], axis=-1).reshape(sizes[c] * beams, 2 * LANES)

    def stage(level, c):
        level_copy(level, c).wait_recv()
        size, extent = sizes[c], sizes[c] * beams
        at = slice(starts[c], starts[c] + size)
        kept = state[level, bit(level), at]
        both = jnp.concatenate([kept, landed[level, at]], axis=1)
        high, low = split(turned(level, c, both))
        m = [merge[level, i, :extent, :extent] for i in range(2)]
        values = dot(m[0], high) + dot(m[0], low) + dot(m[1], high)
        if level + 1 < final:
            publish(level + 1, c, values)
            return
        values = turned(final, c, values.reshape(size, beams, 2 * LANES))
        back = transformed(values, wi_ref).reshape(size, beams, 2 * LANES)
        for k in range(size):
            at = starts[c] + k
            tr, ti = tw_ref[0, at : at + 1, :], tw_ref[1, at : at + 1, :]
            re, im = back[k, :, :LANES], back[k, :, LANES:]
            field[at, :, :LANES] = re * tr - im * ti
            field[at, :, LANES:] = im * tr + re * ti
        if twice:

            @pl.when(inner(me) == 1)
            def _():
                extra_copy(c).start()

    def extra_copy(c):
        at = pl.ds(starts[c], sizes[c])
        return pltpu.make_async_remote_copy(
            src_ref=field.at[at, pl.ds(half, half)], dst_ref=extra.at[at],
            send_sem=extra_send, recv_sem=extra_recv,
            device_id={"sub": facing(me)}, device_id_type=pl.DeviceIdType.MESH,
        )

    def turn_order(at):
        level, c = at
        return (GAP * level * outer / 32 + starts[c], level)

    def spectrum(c):
        lines = field[starts[c] : starts[c] + sizes[c]].reshape(sizes[c] * beams, 2 * LANES)
        values = transformed(lines, wf_ref)
        if c == 0:
            pl.semaphore_wait(barrier, n - 1)
        publish(0, c, values)

    loads[later + 1].wait()
    for c in range(AHEAD):
        spectrum(c)
    for load in loads[later + 2 : later + 6]:
        load.wait()
    write_card()
    for v in range(1, n):
        card_copy(v).start()
    write_columns()
    prepare(0)
    for c in range(chunks):
        stage(0, c)
        if c + AHEAD < chunks:
            spectrum(c + AHEAD)
    loads[later + 6].wait()
    ready = 1
    for level, c in sorted(((a, b) for a in range(1, final) for b in range(chunks)), key=turn_order):
        while ready <= (final if level == final - 1 else level):
            prepare(ready)
            ready += 1
        stage(level, c)
        if ready < final:
            prepare(ready)
            ready += 1

    for g in range(beams // 8):
        at = slice(g * 8, g * 8 + 8)
        lines = [(field[k, at, :LANES], field[k, at, LANES:]) for k in range(outer)]
        for q, pair in enumerate(butterflies(lines, 1)):
            for p in range(2):
                if groups == 1:
                    sendbuf[q // per, q % per, p, at] = pair[p]
                else:
                    field[q, at, p * LANES : (p + 1) * LANES] = pair[p]
    if groups > 1:
        for q in range(outer):
            for p in range(2):
                line = field[q, :, p * LANES : (p + 1) * LANES]
                for g in range(groups):
                    parts = [line[s * rows : (s + 1) * rows, g * width : (g + 1) * width] for s in range(groups)]
                    sendbuf[q * groups + g, 0, p] = jnp.concatenate(parts, axis=1)

    def turn_send_to(there, rows):
        lines = pl.ds(0, rows)
        pltpu.make_async_remote_copy(
            src_ref=sendbuf.at[there, :, :, lines], dst_ref=gathered.at[me, :, :, lines],
            send_sem=turn_send, recv_sem=turn_recv,
            device_id={"sub": there}, device_id_type=pl.DeviceIdType.MESH,
        ).start()

    for v in range(1, n):
        there = (me + v) % n
        if not twice:
            turn_send_to(there, rows)
            continue
        part = inner(me) * ((bit(final) + bit_of(there, final)) % 2)
        pl.when(part == 0)(functools.partial(turn_send_to, there, rows))
        pl.when(part == 1)(functools.partial(turn_send_to, there, half))

    def share_copy(slot, target):
        return pltpu.make_async_remote_copy(
            src_ref=packed.at[slot], dst_ref=gathered.at[facing(me), :, :, pl.ds(half, half)],
            send_sem=share_send, recv_sem=share_recv,
            device_id={"sub": target}, device_id_type=pl.DeviceIdType.MESH,
        )

    def shared(count):
        return all_of(packed.at[pl.ds(0, count)], packed.at[pl.ds(0, count)], share_send, share_recv)

    def turned_slabs(count):
        return all_of(sendbuf.at[pl.ds(0, count)], gathered.at[pl.ds(0, count)], turn_send, turn_recv)

    if twice:

        @pl.when(inner(me) == 1)
        def _():
            all_of(extra, extra, extra_send, extra_recv).wait_recv()
            lines = [(extra[k, :, :LANES], extra[k, :, LANES:]) for k in range(outer)]
            even, odd = butterflies(lines[0::2], 1), butterflies(lines[1::2], 1)
            sign = (1 - 2 * bit(final)).astype(F32)
            for k in range(outer // 2):
                angle = 2.0 * math.pi * k / outer
                turn = times_constant(odd[k], complex(math.cos(angle), math.sin(angle)))
                for p in range(2):
                    packed[k // per, k % per, p] = even[k][p] + sign * turn[p]

        for slot in range(n // 2):
            target = bit(final) * (n // 2) + slot
            pl.when(inner(me) * jnp.where(target == me, 0, 1) == 1)(share_copy(slot, target).start)

        @pl.when(inner(me) == 1)
        def _():
            gathered[facing(me), :, :, half:] = packed[me % (n // 2)]

    gathered[me] = sendbuf[me]
    cards[me] = card[...]
    all_of(cards.at[pl.ds(0, n - 2)], cards.at[pl.ds(0, n - 2)], card_send, card_recv).wait_recv()
    families = n // 16
    if groups == 1:
        lane = lax.broadcasted_iota(jnp.int32, (half, LANES), 1)
        for h in range(2):
            for g in range(families):
                tiles = []
                for side in range(2):
                    for f in range(8):
                        values = cards[h * (n // 2) + g * 8 + f]
                        child = side ^ h
                        moved = pltpu.roll(values, (f - child) * beams % LANES, 1)
                        tiles.append(jnp.where((lane >= f * beams) & (lane < (f + 1) * beams), moved, 0.0))
                high, low = split(jnp.concatenate(tiles, axis=0))
                more[h, g, 0] = high
                more[h, g, 1] = low
    for level in range(final):
        sent = state.at[level, 1 - bit(level)]
        all_of(sent, landed.at[level], level_send.at[level], level_recv.at[level, 0]).wait_send()
    all_of(cards.at[pl.ds(0, n - 1)], cards.at[pl.ds(0, n - 1)], card_send, card_recv).wait_send()
    if groups > 1:
        more[...] = cards[...]
    if not twice:
        turned_slabs(n - 1).wait_recv()
        turned_slabs(n - 1).wait_send()
        return
    turned_slabs(n - 1 - n // 16).wait_recv()

    @pl.when(inner(me) == 0)
    def _():
        shared(n // 8).wait_recv()
        turned_slabs(n - 1).wait_send()

    @pl.when(inner(me) == 1)
    def _():
        shared(n // 8 - 1).wait_recv()
        turned_slabs(n - 1 - n // 4).wait_send()
        shared(n // 2 - 1).wait_send()
        all_of(extra, extra, extra_send, extra_recv).wait_send()


def finish(cfg, gathered, last, out_hbm, out_ref, sem):
    n, per, half = cfg["n"], cfg["per"], cfg["beams"] // 2
    families = n // 16
    stores = []
    for r in range(per):
        for p in range(2):
            for h in range(2):
                for g in range(families):
                    sides = [
                        gathered[at : at + 8, r, p, h * half : (h + 1) * half].reshape(LANES // 2, LANES)
                        for at in (g * 8, n // 2 + g * 8)
                    ]
                    high, low = split(jnp.concatenate(sides, axis=0).T)
                    value = dot(high, last[h, g, 0]) + dot(low, last[h, g, 0]) + dot(high, last[h, g, 1])
                    at = (h * families + g) * LANES
                    out_ref[p, r * LANES : (r + 1) * LANES, at : at + LANES] = value
            at = (p, pl.ds(r * LANES, LANES))
            stores.append(pltpu.make_async_copy(out_ref.at[at], out_hbm.at[at], sem.at[r, p]))
            stores[-1].start()
    for store in stores:
        store.wait()


def real_form(length, direction, factor):
    index = np.arange(length)
    turns = (index[:, None] * index[None, :] % length) * (direction * 2.0 * np.pi / length)
    c, s = np.cos(turns) * factor, np.sin(turns) * factor
    full = np.block([[c, s], [-s, c]]).astype(np.float32)
    high = np.asarray(full, dtype=jnp.bfloat16)
    low = np.asarray(full - high.astype(np.float32), dtype=jnp.bfloat16)
    return np.stack([high, low])


def body(n, sub_images, shift_table, phase_table, offset_table, weight_table):
    beams, bins = sub_images.shape[1], sub_images.shape[2]
    levels, taps = shift_table.shape[0], weight_table.shape[3]
    outer = bins // LANES
    share = bins // n
    per = max(1, share // LANES)
    groups = max(1, LANES // share)
    sizes = tuple(part * outer // sum(CHUNKS) for part in CHUNKS)
    rows = beams // groups
    cfg = dict(n=n, levels=levels, outer=outer, beams=beams, sizes=sizes, per=per, groups=groups,
               width=min(share, LANES), rows=rows, taps=taps, twice=groups == 1 and levels > 2)
    turns = np.arange(outer)[:, None] * np.arange(LANES)[None, :] * (2.0 * np.pi / bins)
    twiddle = np.stack([np.cos(turns), np.sin(turns)]).astype(np.float32)
    half = beams // 2
    blocks = -(-levels * (6 + 2 * taps) // LANES)
    shapes = [((n, per, 2, rows, LANES), F32)]
    shapes.append(((2, n // 16, 2, LANES, LANES), BF16) if groups == 1 else ((n, half, LANES), F32))
    held = sum(math.prod(shape) * jnp.dtype(kind).itemsize for shape, kind in shapes)
    vmem = pl.BlockSpec(memory_space=pltpu.VMEM)
    operands = (
        sub_images, shift_table, phase_table, offset_table, weight_table, jnp.asarray(real_form(LANES, -1, 1.0)),
        jnp.asarray(real_form(LANES, 1, 1.0 / bins)), jnp.asarray(twiddle),
    )
    result = pl.pallas_call(
        functools.partial(kernel, cfg),
        name="merges",
        out_shape=[pltpu.VMEM(*shape) for shape in shapes],
        in_specs=[pl.BlockSpec(memory_space=pltpu.HBM)] * 8,
        out_specs=[vmem] * len(shapes),
        scratch_shapes=[
            *[pltpu.VMEM(a.shape, a.dtype) for a in operands],
            pltpu.VMEM((outer, beams, 2 * LANES), F32),
            pltpu.VMEM((levels - 1, 2, outer, half, 2 * LANES), F32),
            pltpu.VMEM((levels - 1, outer, half, 2 * LANES), F32),
            pltpu.VMEM((blocks * LANES, LANES), F32),
            pltpu.VMEM((blocks, LANES, LANES), F32),
            pltpu.VMEM((levels, 4, beams, LANES), F32),
            pltpu.VMEM((levels - 1, 2, max(sizes) * beams, max(sizes) * beams), BF16),
            pltpu.VMEM((n, per, 2, rows, LANES), F32),
            pltpu.VMEM((half, LANES), F32),
            pltpu.VMEM((n, half, LANES), F32),
            pltpu.VMEM((outer, half, 2 * LANES), F32),
            pltpu.VMEM((n // 2, per, 2, half, LANES), F32),
            pltpu.SemaphoreType.DMA((beams // 8 + 7,)),
            pltpu.SemaphoreType.DMA((levels - 1,)),
            pltpu.SemaphoreType.DMA((levels - 1, len(sizes))),
            pltpu.SemaphoreType.DMA((9,)),
        ],
        compiler_params=pltpu.CompilerParams(
            collective_id=0, has_side_effects=True, vmem_limit_bytes=VMEM - held
        ),
    )(*operands)
    if groups == 1:
        shape = (2, per * LANES, n * beams)
        return pl.pallas_call(
            functools.partial(finish, cfg),
            name="finish",
            out_shape=jax.ShapeDtypeStruct(shape, F32),
            in_specs=[vmem] * 2,
            out_specs=pl.BlockSpec(memory_space=pltpu.HBM),
            scratch_shapes=[pltpu.VMEM(shape, F32), pltpu.SemaphoreType.DMA((per, 2))],
            compiler_params=pltpu.CompilerParams(vmem_limit_bytes=24000000),
        )(*result)
    pieces = result[0].reshape(n, 2, rows, groups, share).transpose(1, 4, 0, 3, 2)
    pieces = pieces.reshape(2, share, 2, n // 2, 2, half)
    blocks = result[1][:, :, : 2 * beams].reshape(2, n // 2, half, 2, beams)
    sums = []
    for h in range(2):
        total = 0.0
        for child in range(2):
            total = total + jnp.einsum(
                "pqim,imj->pqij", pieces[:, :, h ^ child, :, h], blocks[h, :, :, child], precision=lax.Precision.HIGHEST
            )
        sums.append(total)
    return jnp.stack(sums, axis=2).reshape(2, share, n * beams)


def solution(mesh):
    placed = (
        P(None, ("img", "sub"), None),
        P(None, "sub", None, None),
        P(None, "sub", None, None),
        P(None, "sub", None, None),
        P(None, "sub", None, None, None),
    )
    return jax.shard_map(
        functools.partial(body, mesh.shape["sub"]),
        mesh=mesh, in_specs=placed, out_specs=P(None, ("img", "sub"), None), check_vma=False,
    )
```

```python
import functools
import math

import jax
import jax.numpy as jnp
import numpy as np
from jax import lax
from jax.experimental import pallas as pl
from jax.experimental.pallas import tpu as pltpu
from jax.sharding import PartitionSpec as P

LANES = 128
CHUNKS = (1, 2, 2, 1, 1, 1)
AHEAD = 3
GAP = 26
TOGETHER = 2
VMEM = 67043328 - (3 << 16)
F32 = jnp.float32
BF16 = jnp.bfloat16


def split(values):
    high = values.astype(BF16)
    low = (values - high.astype(F32)).astype(BF16)
    return high, low


def dot(left, right):
    return jnp.dot(left, right, preferred_element_type=F32)


def times_constant(pair, constant):
    real_part, imag_part = pair
    c, s = constant.real, constant.imag
    if abs(s) < 1e-12:
        return pair if c > 0 else (-real_part, -imag_part)
    if abs(c) < 1e-12:
        return (-imag_part, real_part) if s > 0 else (imag_part, -real_part)
    if abs(abs(c) - abs(s)) < 1e-12:
        h = abs(c)
        a = real_part if c > 0 else -real_part
        b = imag_part if s > 0 else -imag_part
        e = real_part if s > 0 else -real_part
        f = imag_part if c > 0 else -imag_part
        return (a - b) * h, (e + f) * h
    return real_part * c - imag_part * s, real_part * s + imag_part * c


def butterflies(rows, direction):
    n = len(rows)
    if n == 1:
        return rows
    even = butterflies(rows[0::2], direction)
    odd = butterflies(rows[1::2], direction)
    first, second = [], []
    for k in range(n // 2):
        angle = direction * 2.0 * math.pi * k / n
        tr, ti = times_constant(odd[k], complex(math.cos(angle), math.sin(angle)))
        er, ei = even[k]
        first.append((er + tr, ei + ti))
        second.append((er - tr, ei - ti))
    return first + second


def kernel(cfg, x_hbm, shift_hbm, phase_hbm, offset_hbm, weight_hbm, wf_hbm, wi_hbm, tw_hbm, *refs):
    gathered, more, refs = refs[0], refs[1], refs[2:]
    (x_ref, shift_ref, phase_ref, offset_ref, weight_ref, wf_ref, wi_ref, tw_ref,
     field, state, landed, raw, columns, tables, merge, sendbuf, card, cards, extra, packed,
     load_sem, level_send, level_recv, pooled) = refs
    turn_send, turn_recv, card_send, card_recv, facing_recv, extra_send, extra_recv, share_send, share_recv = (
        pooled.at[i] for i in range(9)
    )
    n, levels, outer, beams, sizes = cfg["n"], cfg["levels"], cfg["outer"], cfg["beams"], cfg["sizes"]
    per, groups, width, rows = cfg["per"], cfg["groups"], cfg["width"], cfg["rows"]
    half = beams // 2
    chunks = len(sizes)
    starts = [sum(sizes[:c]) for c in range(chunks)]
    most = max(sizes)
    extent = most * beams
    taps = cfg["taps"]
    total = outer * LANES
    final = levels - 1
    me = lax.axis_index("sub")

    twice = cfg["twice"]

    def bit_of(device, level):
        return (device // (1 << level)) % 2

    def bit(level):
        return bit_of(me, level)

    def inner(device):
        return (bit_of(device, final) + bit_of(device, final - 1)) % 2 * bit_of(device, 0)

    def facing(device):
        for level in (final - 1, final):
            device = device + (1 - 2 * bit_of(device, level)) * (1 << level)
        return device

    def across(mask):
        other = me
        for level in range(levels):
            if mask >> level & 1:
                other = other + (1 - 2 * bit(level)) * (1 << level)
        return other

    pairs = [(x_hbm.at[:, pl.ds(g * 8, 8)], x_ref.at[:, pl.ds(g * 8, 8)]) for g in range(beams // 8)]
    pairs += [(tw_hbm, tw_ref), (wf_hbm, wf_ref), (shift_hbm, shift_ref), (phase_hbm, phase_ref),
              (offset_hbm, offset_ref), (weight_hbm, weight_ref), (wi_hbm, wi_ref)]
    loads = [pltpu.make_async_copy(src, dst, load_sem.at[i]) for i, (src, dst) in enumerate(pairs)]
    for load in loads:
        load.start()

    barrier = pltpu.get_barrier_semaphore()
    for mask in range(1, n):
        pl.semaphore_signal(barrier, inc=1, device_id={"sub": across(mask)}, device_id_type=pl.DeviceIdType.MESH)

    later = beams // 8
    for g in range(beams // 8):
        loads[g].wait()
        if g == 0:
            loads[later].wait()
        lines = [
            tuple(x_ref[p, g * 8 : g * 8 + 8, q * LANES : (q + 1) * LANES] for p in range(2)) for q in range(outer)
        ]
        for k, (re, im) in enumerate(butterflies(lines, -1)):
            tr, ti = tw_ref[0, k : k + 1, :], tw_ref[1, k : k + 1, :]
            field[k, g * 8 : g * 8 + 8, :LANES] = re * tr + im * ti
            field[k, g * 8 : g * 8 + 8, LANES:] = im * tr - re * ti

    def all_of(source, target, send, recv):
        return pltpu.make_async_remote_copy(
            src_ref=source, dst_ref=target, send_sem=send, recv_sem=recv,
            device_id={"sub": across(1)}, device_id_type=pl.DeviceIdType.MESH,
        )

    def card_copy(v):
        there = (me + v) % n
        return pltpu.make_async_remote_copy(
            src_ref=card, dst_ref=cards.at[me], send_sem=card_send, recv_sem=facing_recv if v == n // 2 else card_recv,
            device_id={"sub": there}, device_id_type=pl.DeviceIdType.MESH,
        )

    def write_card():
        place = lax.broadcasted_iota(jnp.int32, (half, beams), 0)
        blocks = []
        for child in range(2):
            first = offset_ref[final, 0, child : child + 1, :]
            block = jnp.zeros((half, beams), F32)
            for t in range(taps):
                block = block + jnp.where(place == first + t, weight_ref[final, 0, child, t : t + 1, :], 0.0)
            blocks.append(block)
        eye = lax.broadcasted_iota(jnp.int32, (half, half), 0) == lax.broadcasted_iota(jnp.int32, (half, half), 1)
        for row in (shift_ref[final, 0, 1:2, :].astype(F32), phase_ref[final, 0, 1:2, :]):
            blocks.append(jnp.sum(jnp.where(eye, row, 0.0), axis=1, keepdims=True))
        blocks.append(jnp.zeros((half, LANES - 2 * beams - 2), F32))
        card[...] = jnp.concatenate(blocks, axis=1)

    count = 6 + 2 * taps

    def write_columns():
        raw[...] = jnp.zeros_like(raw)
        for level in range(levels):
            at = level * count
            raw[at : at + 2, :half] = shift_ref[level, 0].astype(F32)
            raw[at + 2 : at + 4, :half] = phase_ref[level, 0]
            raw[at + 4 : at + 6, :beams] = offset_ref[level, 0].astype(F32)
            for child in range(2):
                raw[at + 6 + child * taps : at + 6 + (child + 1) * taps, :beams] = weight_ref[level, 0, child]
        for i in range(raw.shape[0] // LANES):
            columns[i] = raw[i * LANES : (i + 1) * LANES].T

    def prepare(level):
        def column(row, extent):
            at = level * count + row
            return columns[at // LANES, :extent, at % LANES : at % LANES + 1]

        lane = lax.broadcasted_iota(jnp.int32, (beams, LANES), 1)
        shifts = [column(child, half) for child in range(2)]
        phases = [column(2 + child, half) for child in range(2)]
        if level == final:
            opposite = (me + n // 2) % n
            all_of(card, cards.at[opposite], card_send, facing_recv).wait_recv()
            other = cards[opposite]
            own_first = bit(final) == 0
            a, b = shifts[0], other[:, 2 * beams : 2 * beams + 1]
            shifts = [jnp.where(own_first, a, b), jnp.where(own_first, b, a)]
            a, b = phases[0], other[:, 2 * beams + 1 : 2 * beams + 2]
            phases = [jnp.where(own_first, a, b), jnp.where(own_first, b, a)]
        shift = jnp.concatenate(shifts, axis=0).astype(jnp.int32)
        phase = jnp.concatenate(phases, axis=0)
        signed = jnp.where(lane >= LANES // 2, lane - LANES, lane) * outer
        unit = 2.0 * math.pi / (4 * total)
        coarse = phase - ((signed * shift) & (4 * total - 1)).astype(F32) * unit
        fine = ((lane * shift) & (4 * total - 1)).astype(F32) * (-unit)
        tables[level, 0] = jnp.cos(coarse)
        tables[level, 1] = jnp.sin(coarse)
        tables[level, 2] = jnp.cos(fine)
        tables[level, 3] = jnp.sin(fine)
        if level == final:
            return
        wide = lax.broadcasted_iota(jnp.int32, (beams, extent), 1)
        mask = (
            lax.broadcasted_iota(jnp.int32, (extent, extent), 0) // beams
            == lax.broadcasted_iota(jnp.int32, (extent, extent), 1) // beams
        )
        slot = wide % beams
        second = slot >= half
        place = (slot % half).astype(F32)
        first = jnp.where(second, column(5, beams), column(4, beams))
        block = jnp.zeros((beams, extent), F32)
        for t in range(taps):
            weight = jnp.where(second, column(6 + taps + t, beams), column(6 + t, beams))
            block = block + jnp.where(place == first + t, weight, 0.0)
        tiled = jnp.concatenate([block] * most, axis=0)
        high, low = split(jnp.where(mask, tiled, 0.0))
        merge[level, 0] = high
        merge[level, 1] = low

    def level_copy(level, c):
        return pltpu.make_async_remote_copy(
            src_ref=state.at[level, 1 - bit(level), pl.ds(starts[c], sizes[c])],
            dst_ref=landed.at[level, pl.ds(starts[c], sizes[c])],
            send_sem=level_send.at[level],
            recv_sem=level_recv.at[level, c],
            device_id={"sub": across(1 << level)},
            device_id_type=pl.DeviceIdType.MESH,
        )

    def publish(level, c, values):
        values = values.reshape(sizes[c], 2, half, 2 * LANES)
        for h in range(2):
            state[level, h, starts[c] : starts[c] + sizes[c]] = values[:, h]
        level_copy(level, c).start()

    def transformed(values, w_ref):
        high, low = split(values)
        return dot(high, w_ref[0]) + dot(low, w_ref[0]) + dot(high, w_ref[1])

    def turned(level, c, both):
        fr, fi = [], []
        cr, ci = tables[level, 0], tables[level, 1]
        sr, si = tables[level, 2], tables[level, 3]
        for k in range(starts[c], starts[c] + sizes[c]):
            ar, ai = sr[:, k : k + 1], si[:, k : k + 1]
            fr.append(cr * ar - ci * ai)
            fi.append(cr * ai + ci * ar)
        fr, fi = jnp.stack(fr), jnp.stack(fi)
        zr, zi = both[..., :LANES], both[..., LANES:]
        return jnp.concatenate([zr * fr - zi * fi, zr * fi + zi * fr], axis=-1).reshape(sizes[c] * beams, 2 * LANES)

    def stage(level, c):
        level_copy(level, c).wait_recv()
        size, extent = sizes[c], sizes[c] * beams
        at = slice(starts[c], starts[c] + size)
        kept = state[level, bit(level), at]
        both = jnp.concatenate([kept, landed[level, at]], axis=1)
        high, low = split(turned(level, c, both))
        m = [merge[level, i, :extent, :extent] for i in range(2)]
        values = dot(m[0], high) + dot(m[0], low) + dot(m[1], high)
        if level + 1 < final:
            publish(level + 1, c, values)
            return
        values = turned(final, c, values.reshape(size, beams, 2 * LANES))
        back = transformed(values, wi_ref).reshape(size, beams, 2 * LANES)
        for k in range(size):
            at = starts[c] + k
            tr, ti = tw_ref[0, at : at + 1, :], tw_ref[1, at : at + 1, :]
            re, im = back[k, :, :LANES], back[k, :, LANES:]
            field[at, :, :LANES] = re * tr - im * ti
            field[at, :, LANES:] = im * tr + re * ti
        if twice:

            @pl.when(inner(me) == 1)
            def _():
                extra_copy(c).start()

    def extra_copy(c):
        at = pl.ds(starts[c], sizes[c])
        return pltpu.make_async_remote_copy(
            src_ref=field.at[at, pl.ds(half, half)], dst_ref=extra.at[at],
            send_sem=extra_send, recv_sem=extra_recv,
            device_id={"sub": facing(me)}, device_id_type=pl.DeviceIdType.MESH,
        )

    def turn_order(at):
        level, c = at
        return (GAP * level * outer / 32 + starts[c], level)

    def spectrum(c):
        lines = field[starts[c] : starts[c] + sizes[c]].reshape(sizes[c] * beams, 2 * LANES)
        values = transformed(lines, wf_ref)
        if c == 0:
            pl.semaphore_wait(barrier, n - 1)
        publish(0, c, values)

    loads[later + 1].wait()
    for c in range(AHEAD):
        spectrum(c)
    for load in loads[later + 2 : later + 6]:
        load.wait()
    write_card()
    for v in range(1, n):
        card_copy(v).start()
    write_columns()
    prepare(0)
    for c in range(chunks):
        stage(0, c)
        if c + AHEAD < chunks:
            spectrum(c + AHEAD)
    loads[later + 6].wait()
    ready = 1
    for level, c in sorted(((a, b) for a in range(1, final) for b in range(chunks)), key=turn_order):
        while ready <= (final if level == final - 1 else level):
            prepare(ready)
            ready += 1
        stage(level, c)
        if ready < final:
            prepare(ready)
            ready += 1

    for g in range(beams // 8):
        at = slice(g * 8, g * 8 + 8)
        lines = [(field[k, at, :LANES], field[k, at, LANES:]) for k in range(outer)]
        for q, pair in enumerate(butterflies(lines, 1)):
            for p in range(2):
                if groups == 1:
                    sendbuf[q // per, q % per, p, at] = pair[p]
                else:
                    field[q, at, p * LANES : (p + 1) * LANES] = pair[p]
    if groups > 1:
        for q in range(outer):
            for p in range(2):
                line = field[q, :, p * LANES : (p + 1) * LANES]
                for g in range(groups):
                    parts = [line[s * rows : (s + 1) * rows, g * width : (g + 1) * width] for s in range(groups)]
                    sendbuf[q * groups + g, 0, p] = jnp.concatenate(parts, axis=1)

    def turn_send_to(there, rows):
        lines = pl.ds(0, rows)
        pltpu.make_async_remote_copy(
            src_ref=sendbuf.at[there, :, :, lines], dst_ref=gathered.at[me, :, :, lines],
            send_sem=turn_send, recv_sem=turn_recv,
            device_id={"sub": there}, device_id_type=pl.DeviceIdType.MESH,
        ).start()

    for v in range(1, n):
        there = (me + v) % n
        if not twice:
            turn_send_to(there, rows)
            continue
        part = inner(me) * ((bit(final) + bit_of(there, final)) % 2)
        pl.when(part == 0)(functools.partial(turn_send_to, there, rows))
        pl.when(part == 1)(functools.partial(turn_send_to, there, half))

    def share_copy(slot, target):
        return pltpu.make_async_remote_copy(
            src_ref=packed.at[slot], dst_ref=gathered.at[facing(me), :, :, pl.ds(half, half)],
            send_sem=share_send, recv_sem=share_recv,
            device_id={"sub": target}, device_id_type=pl.DeviceIdType.MESH,
        )

    def shared(count):
        return all_of(packed.at[pl.ds(0, count)], packed.at[pl.ds(0, count)], share_send, share_recv)

    def turned_slabs(count):
        return all_of(sendbuf.at[pl.ds(0, count)], gathered.at[pl.ds(0, count)], turn_send, turn_recv)

    if twice:

        @pl.when(inner(me) == 1)
        def _():
            all_of(extra, extra, extra_send, extra_recv).wait_recv()
            lines = [(extra[k, :, :LANES], extra[k, :, LANES:]) for k in range(outer)]
            even, odd = butterflies(lines[0::2], 1), butterflies(lines[1::2], 1)
            sign = (1 - 2 * bit(final)).astype(F32)
            for k in range(outer // 2):
                angle = 2.0 * math.pi * k / outer
                turn = times_constant(odd[k], complex(math.cos(angle), math.sin(angle)))
                for p in range(2):
                    packed[k // per, k % per, p] = even[k][p] + sign * turn[p]

        for slot in range(n // 2):
            target = bit(final) * (n // 2) + slot
            pl.when(inner(me) * jnp.where(target == me, 0, 1) == 1)(share_copy(slot, target).start)

        @pl.when(inner(me) == 1)
        def _():
            gathered[facing(me), :, :, half:] = packed[me % (n // 2)]

    gathered[me] = sendbuf[me]
    cards[me] = card[...]
    all_of(cards.at[pl.ds(0, n - 2)], cards.at[pl.ds(0, n - 2)], card_send, card_recv).wait_recv()
    families = n // 16
    if groups == 1:
        lane = lax.broadcasted_iota(jnp.int32, (half, LANES), 1)
        for h in range(2):
            for g in range(families):
                tiles = []
                for side in range(2):
                    for f in range(8):
                        values = cards[h * (n // 2) + g * 8 + f]
                        child = side ^ h
                        moved = pltpu.roll(values, (f - child) * beams % LANES, 1)
                        tiles.append(jnp.where((lane >= f * beams) & (lane < (f + 1) * beams), moved, 0.0))
                high, low = split(jnp.concatenate(tiles, axis=0))
                more[h, g, 0] = high
                more[h, g, 1] = low
    for level in range(final):
        sent = state.at[level, 1 - bit(level)]
        all_of(sent, landed.at[level], level_send.at[level], level_recv.at[level, 0]).wait_send()
    all_of(cards.at[pl.ds(0, n - 1)], cards.at[pl.ds(0, n - 1)], card_send, card_recv).wait_send()
    if groups > 1:
        more[...] = cards[...]
    if not twice:
        turned_slabs(n - 1).wait_recv()
        turned_slabs(n - 1).wait_send()
        return
    turned_slabs(n - 1 - n // 16).wait_recv()

    @pl.when(inner(me) == 0)
    def _():
        shared(n // 8).wait_recv()
        turned_slabs(n - 1).wait_send()

    @pl.when(inner(me) == 1)
    def _():
        shared(n // 8 - 1).wait_recv()
        turned_slabs(n - 1 - n // 4).wait_send()
        shared(n // 2 - 1).wait_send()
        all_of(extra, extra, extra_send, extra_recv).wait_send()


def finish(cfg, gathered, last, out_hbm, out_ref, sem):
    n, per, half = cfg["n"], cfg["per"], cfg["beams"] // 2
    families = n // 16
    stores = []
    tiles = [(r, p) for r in range(per) for p in range(2)]
    for first in range(0, len(tiles), TOGETHER):
        group = tiles[first : first + TOGETHER]
        for r, p in group:
            for h in range(2):
                for g in range(families):
                    sides = [
                        gathered[at : at + 8, r, p, h * half : (h + 1) * half].reshape(LANES // 2, LANES)
                        for at in (g * 8, n // 2 + g * 8)
                    ]
                    high, low = split(jnp.concatenate(sides, axis=0).T)
                    value = dot(high, last[h, g, 0]) + dot(low, last[h, g, 0]) + dot(high, last[h, g, 1])
                    at = (h * families + g) * LANES
                    out_ref[p, r * LANES : (r + 1) * LANES, at : at + LANES] = value
        for r, p in group:
            at = (p, pl.ds(r * LANES, LANES))
            stores.append(pltpu.make_async_copy(out_ref.at[at], out_hbm.at[at], sem.at[r, p]))
            stores[-1].start()
    for store in stores:
        store.wait()


def real_form(length, direction, factor):
    index = np.arange(length)
    turns = (index[:, None] * index[None, :] % length) * (direction * 2.0 * np.pi / length)
    c, s = np.cos(turns) * factor, np.sin(turns) * factor
    full = np.block([[c, s], [-s, c]]).astype(np.float32)
    high = np.asarray(full, dtype=jnp.bfloat16)
    low = np.asarray(full - high.astype(np.float32), dtype=jnp.bfloat16)
    return np.stack([high, low])


def body(n, sub_images, shift_table, phase_table, offset_table, weight_table):
    beams, bins = sub_images.shape[1], sub_images.shape[2]
    levels, taps = shift_table.shape[0], weight_table.shape[3]
    outer = bins // LANES
    share = bins // n
    per = max(1, share // LANES)
    groups = max(1, LANES // share)
    sizes = tuple(part * outer // sum(CHUNKS) for part in CHUNKS)
    rows = beams // groups
    cfg = dict(n=n, levels=levels, outer=outer, beams=beams, sizes=sizes, per=per, groups=groups,
               width=min(share, LANES), rows=rows, taps=taps, twice=groups == 1 and levels > 2)
    turns = np.arange(outer)[:, None] * np.arange(LANES)[None, :] * (2.0 * np.pi / bins)
    twiddle = np.stack([np.cos(turns), np.sin(turns)]).astype(np.float32)
    half = beams // 2
    blocks = -(-levels * (6 + 2 * taps) // LANES)
    shapes = [((n, per, 2, rows, LANES), F32)]
    shapes.append(((2, n // 16, 2, LANES, LANES), BF16) if groups == 1 else ((n, half, LANES), F32))
    held = sum(math.prod(shape) * jnp.dtype(kind).itemsize for shape, kind in shapes)
    vmem = pl.BlockSpec(memory_space=pltpu.VMEM)
    operands = (
        sub_images, shift_table, phase_table, offset_table, weight_table, jnp.asarray(real_form(LANES, -1, 1.0)),
        jnp.asarray(real_form(LANES, 1, 1.0 / bins)), jnp.asarray(twiddle),
    )
    result = pl.pallas_call(
        functools.partial(kernel, cfg),
        name="merges",
        out_shape=[pltpu.VMEM(*shape) for shape in shapes],
        in_specs=[pl.BlockSpec(memory_space=pltpu.HBM)] * 8,
        out_specs=[vmem] * len(shapes),
        scratch_shapes=[
            *[pltpu.VMEM(a.shape, a.dtype) for a in operands],
            pltpu.VMEM((outer, beams, 2 * LANES), F32),
            pltpu.VMEM((levels - 1, 2, outer, half, 2 * LANES), F32),
            pltpu.VMEM((levels - 1, outer, half, 2 * LANES), F32),
            pltpu.VMEM((blocks * LANES, LANES), F32),
            pltpu.VMEM((blocks, LANES, LANES), F32),
            pltpu.VMEM((levels, 4, beams, LANES), F32),
            pltpu.VMEM((levels - 1, 2, max(sizes) * beams, max(sizes) * beams), BF16),
            pltpu.VMEM((n, per, 2, rows, LANES), F32),
            pltpu.VMEM((half, LANES), F32),
            pltpu.VMEM((n, half, LANES), F32),
            pltpu.VMEM((outer, half, 2 * LANES), F32),
            pltpu.VMEM((n // 2, per, 2, half, LANES), F32),
            pltpu.SemaphoreType.DMA((beams // 8 + 7,)),
            pltpu.SemaphoreType.DMA((levels - 1,)),
            pltpu.SemaphoreType.DMA((levels - 1, len(sizes))),
            pltpu.SemaphoreType.DMA((9,)),
        ],
        compiler_params=pltpu.CompilerParams(
            collective_id=0, has_side_effects=True, vmem_limit_bytes=VMEM - held
        ),
    )(*operands)
    if groups == 1:
        shape = (2, per * LANES, n * beams)
        return pl.pallas_call(
            functools.partial(finish, cfg),
            name="finish",
            out_shape=jax.ShapeDtypeStruct(shape, F32),
            in_specs=[vmem] * 2,
            out_specs=pl.BlockSpec(memory_space=pltpu.HBM),
            scratch_shapes=[pltpu.VMEM(shape, F32), pltpu.SemaphoreType.DMA((per, 2))],
            compiler_params=pltpu.CompilerParams(vmem_limit_bytes=24000000),
        )(*result)
    pieces = result[0].reshape(n, 2, rows, groups, share).transpose(1, 4, 0, 3, 2)
    pieces = pieces.reshape(2, share, 2, n // 2, 2, half)
    blocks = result[1][:, :, : 2 * beams].reshape(2, n // 2, half, 2, beams)
    sums = []
    for h in range(2):
        total = 0.0
        for child in range(2):
            total = total + jnp.einsum(
                "pqim,imj->pqij", pieces[:, :, h ^ child, :, h], blocks[h, :, :, child], precision=lax.Precision.HIGHEST
            )
        sums.append(total)
    return jnp.stack(sums, axis=2).reshape(2, share, n * beams)


def solution(mesh):
    placed = (
        P(None, ("img", "sub"), None),
        P(None, "sub", None, None),
        P(None, "sub", None, None),
        P(None, "sub", None, None),
        P(None, "sub", None, None, None),
    )
    return jax.shard_map(
        functools.partial(body, mesh.shape["sub"]),
        mesh=mesh, in_specs=placed, out_specs=P(None, ("img", "sub"), None), check_vma=False,
    )
```

```python
import functools
import math

import jax
import jax.numpy as jnp
import numpy as np
from jax import lax
from jax.experimental import pallas as pl
from jax.experimental.pallas import tpu as pltpu
from jax.sharding import PartitionSpec as P

LANES = 128
CHUNKS = (1, 1, 1, 2, 1, 1, 1)
AHEAD = 3
GAP = 26
VMEM = 67043328 - (3 << 16)
F32 = jnp.float32
BF16 = jnp.bfloat16


def split(values):
    high = values.astype(BF16)
    low = (values - high.astype(F32)).astype(BF16)
    return high, low


def dot(left, right):
    return jnp.dot(left, right, preferred_element_type=F32)


def times_constant(pair, constant):
    real_part, imag_part = pair
    c, s = constant.real, constant.imag
    if abs(s) < 1e-12:
        return pair if c > 0 else (-real_part, -imag_part)
    if abs(c) < 1e-12:
        return (-imag_part, real_part) if s > 0 else (imag_part, -real_part)
    if abs(abs(c) - abs(s)) < 1e-12:
        h = abs(c)
        a = real_part if c > 0 else -real_part
        b = imag_part if s > 0 else -imag_part
        e = real_part if s > 0 else -real_part
        f = imag_part if c > 0 else -imag_part
        return (a - b) * h, (e + f) * h
    return real_part * c - imag_part * s, real_part * s + imag_part * c


def butterflies(rows, direction):
    n = len(rows)
    if n == 1:
        return rows
    even = butterflies(rows[0::2], direction)
    odd = butterflies(rows[1::2], direction)
    first, second = [], []
    for k in range(n // 2):
        angle = direction * 2.0 * math.pi * k / n
        tr, ti = times_constant(odd[k], complex(math.cos(angle), math.sin(angle)))
        er, ei = even[k]
        first.append((er + tr, ei + ti))
        second.append((er - tr, ei - ti))
    return first + second


def kernel(cfg, x_hbm, shift_hbm, phase_hbm, offset_hbm, weight_hbm, wf_hbm, wi_hbm, tw_hbm, *refs):
    gathered, more, refs = refs[0], refs[1], refs[2:]
    (x_ref, shift_ref, phase_ref, offset_ref, weight_ref, wf_ref, wi_ref, tw_ref,
     field, state, landed, raw, columns, tables, merge, sendbuf, card, cards, extra, packed,
     load_sem, level_send, level_recv, pooled) = refs
    turn_send, turn_recv, card_send, card_recv, facing_recv, extra_send, extra_recv, share_send, share_recv = (
        pooled.at[i] for i in range(9)
    )
    n, levels, outer, beams, sizes = cfg["n"], cfg["levels"], cfg["outer"], cfg["beams"], cfg["sizes"]
    per, groups, width, rows = cfg["per"], cfg["groups"], cfg["width"], cfg["rows"]
    half = beams // 2
    chunks = len(sizes)
    starts = [sum(sizes[:c]) for c in range(chunks)]
    most = max(sizes)
    extent = most * beams
    taps = cfg["taps"]
    total = outer * LANES
    final = levels - 1
    me = lax.axis_index("sub")

    twice = cfg["twice"]

    def bit_of(device, level):
        return (device // (1 << level)) % 2

    def bit(level):
        return bit_of(me, level)

    def inner(device):
        return (bit_of(device, final) + bit_of(device, final - 1)) % 2 * bit_of(device, 0)

    def facing(device):
        for level in (final - 1, final):
            device = device + (1 - 2 * bit_of(device, level)) * (1 << level)
        return device

    def across(mask):
        other = me
        for level in range(levels):
            if mask >> level & 1:
                other = other + (1 - 2 * bit(level)) * (1 << level)
        return other

    pairs = [(x_hbm.at[:, pl.ds(g * 8, 8)], x_ref.at[:, pl.ds(g * 8, 8)]) for g in range(beams // 8)]
    pairs += [(tw_hbm, tw_ref), (wf_hbm, wf_ref), (shift_hbm, shift_ref), (phase_hbm, phase_ref),
              (offset_hbm, offset_ref), (weight_hbm, weight_ref), (wi_hbm, wi_ref)]
    loads = [pltpu.make_async_copy(src, dst, load_sem.at[i]) for i, (src, dst) in enumerate(pairs)]
    for load in loads:
        load.start()

    barrier = pltpu.get_barrier_semaphore()
    for mask in range(1, n):
        pl.semaphore_signal(barrier, inc=1, device_id={"sub": across(mask)}, device_id_type=pl.DeviceIdType.MESH)

    later = beams // 8
    for g in range(beams // 8):
        loads[g].wait()
        if g == 0:
            loads[later].wait()
        lines = [
            tuple(x_ref[p, g * 8 : g * 8 + 8, q * LANES : (q + 1) * LANES] for p in range(2)) for q in range(outer)
        ]
        for k, (re, im) in enumerate(butterflies(lines, -1)):
            tr, ti = tw_ref[0, k : k + 1, :], tw_ref[1, k : k + 1, :]
            field[k, g * 8 : g * 8 + 8, :LANES] = re * tr + im * ti
            field[k, g * 8 : g * 8 + 8, LANES:] = im * tr - re * ti

    def all_of(source, target, send, recv):
        return pltpu.make_async_remote_copy(
            src_ref=source, dst_ref=target, send_sem=send, recv_sem=recv,
            device_id={"sub": across(1)}, device_id_type=pl.DeviceIdType.MESH,
        )

    def card_copy(v):
        there = (me + v) % n
        return pltpu.make_async_remote_copy(
            src_ref=card, dst_ref=cards.at[me], send_sem=card_send, recv_sem=facing_recv if v == n // 2 else card_recv,
            device_id={"sub": there}, device_id_type=pl.DeviceIdType.MESH,
        )

    def write_card():
        place = lax.broadcasted_iota(jnp.int32, (half, beams), 0)
        blocks = []
        for child in range(2):
            first = offset_ref[final, 0, child : child + 1, :]
            block = jnp.zeros((half, beams), F32)
            for t in range(taps):
                block = block + jnp.where(place == first + t, weight_ref[final, 0, child, t : t + 1, :], 0.0)
            blocks.append(block)
        eye = lax.broadcasted_iota(jnp.int32, (half, half), 0) == lax.broadcasted_iota(jnp.int32, (half, half), 1)
        for row in (shift_ref[final, 0, 1:2, :].astype(F32), phase_ref[final, 0, 1:2, :]):
            blocks.append(jnp.sum(jnp.where(eye, row, 0.0), axis=1, keepdims=True))
        blocks.append(jnp.zeros((half, LANES - 2 * beams - 2), F32))
        card[...] = jnp.concatenate(blocks, axis=1)

    count = 6 + 2 * taps

    def write_columns():
        raw[...] = jnp.zeros_like(raw)
        for level in range(levels):
            at = level * count
            raw[at : at + 2, :half] = shift_ref[level, 0].astype(F32)
            raw[at + 2 : at + 4, :half] = phase_ref[level, 0]
            raw[at + 4 : at + 6, :beams] = offset_ref[level, 0].astype(F32)
            for child in range(2):
                raw[at + 6 + child * taps : at + 6 + (child + 1) * taps, :beams] = weight_ref[level, 0, child]
        for i in range(raw.shape[0] // LANES):
            columns[i] = raw[i * LANES : (i + 1) * LANES].T

    def prepare(level):
        def column(row, extent):
            at = level * count + row
            return columns[at // LANES, :extent, at % LANES : at % LANES + 1]

        lane = lax.broadcasted_iota(jnp.int32, (beams, LANES), 1)
        shifts = [column(child, half) for child in range(2)]
        phases = [column(2 + child, half) for child in range(2)]
        if level == final:
            opposite = (me + n // 2) % n
            all_of(card, cards.at[opposite], card_send, facing_recv).wait_recv()
            other = cards[opposite]
            own_first = bit(final) == 0
            a, b = shifts[0], other[:, 2 * beams : 2 * beams + 1]
            shifts = [jnp.where(own_first, a, b), jnp.where(own_first, b, a)]
            a, b = phases[0], other[:, 2 * beams + 1 : 2 * beams + 2]
            phases = [jnp.where(own_first, a, b), jnp.where(own_first, b, a)]
        shift = jnp.concatenate(shifts, axis=0).astype(jnp.int32)
        phase = jnp.concatenate(phases, axis=0)
        signed = jnp.where(lane >= LANES // 2, lane - LANES, lane) * outer
        unit = 2.0 * math.pi / (4 * total)
        coarse = phase - ((signed * shift) & (4 * total - 1)).astype(F32) * unit
        fine = ((lane * shift) & (4 * total - 1)).astype(F32) * (-unit)
        tables[level, 0] = jnp.cos(coarse)
        tables[level, 1] = jnp.sin(coarse)
        tables[level, 2] = jnp.cos(fine)
        tables[level, 3] = jnp.sin(fine)
        if level == final:
            return
        wide = lax.broadcasted_iota(jnp.int32, (beams, extent), 1)
        mask = (
            lax.broadcasted_iota(jnp.int32, (extent, extent), 0) // beams
            == lax.broadcasted_iota(jnp.int32, (extent, extent), 1) // beams
        )
        slot = wide % beams
        second = slot >= half
        place = (slot % half).astype(F32)
        first = jnp.where(second, column(5, beams), column(4, beams))
        block = jnp.zeros((beams, extent), F32)
        for t in range(taps):
            weight = jnp.where(second, column(6 + taps + t, beams), column(6 + t, beams))
            block = block + jnp.where(place == first + t, weight, 0.0)
        tiled = jnp.concatenate([block] * most, axis=0)
        high, low = split(jnp.where(mask, tiled, 0.0))
        merge[level, 0] = high
        merge[level, 1] = low

    def level_copy(level, c):
        return pltpu.make_async_remote_copy(
            src_ref=state.at[level, 1 - bit(level), pl.ds(starts[c], sizes[c])],
            dst_ref=landed.at[level, pl.ds(starts[c], sizes[c])],
            send_sem=level_send.at[level],
            recv_sem=level_recv.at[level, c],
            device_id={"sub": across(1 << level)},
            device_id_type=pl.DeviceIdType.MESH,
        )

    def publish(level, c, values):
        values = values.reshape(sizes[c], 2, half, 2 * LANES)
        for h in range(2):
            state[level, h, starts[c] : starts[c] + sizes[c]] = values[:, h]
        level_copy(level, c).start()

    def transformed(values, w_ref):
        high, low = split(values)
        return dot(high, w_ref[0]) + dot(low, w_ref[0]) + dot(high, w_ref[1])

    def turned(level, c, both):
        fr, fi = [], []
        cr, ci = tables[level, 0], tables[level, 1]
        sr, si = tables[level, 2], tables[level, 3]
        for k in range(starts[c], starts[c] + sizes[c]):
            ar, ai = sr[:, k : k + 1], si[:, k : k + 1]
            fr.append(cr * ar - ci * ai)
            fi.append(cr * ai + ci * ar)
        fr, fi = jnp.stack(fr), jnp.stack(fi)
        zr, zi = both[..., :LANES], both[..., LANES:]
        return jnp.concatenate([zr * fr - zi * fi, zr * fi + zi * fr], axis=-1).reshape(sizes[c] * beams, 2 * LANES)

    def stage(level, c):
        level_copy(level, c).wait_recv()
        size, extent = sizes[c], sizes[c] * beams
        at = slice(starts[c], starts[c] + size)
        kept = state[level, bit(level), at]
        both = jnp.concatenate([kept, landed[level, at]], axis=1)
        high, low = split(turned(level, c, both))
        m = [merge[level, i, :extent, :extent] for i in range(2)]
        values = dot(m[0], high) + dot(m[0], low) + dot(m[1], high)
        if level + 1 < final:
            publish(level + 1, c, values)
            return
        values = turned(final, c, values.reshape(size, beams, 2 * LANES))
        back = transformed(values, wi_ref).reshape(size, beams, 2 * LANES)
        for k in range(size):
            at = starts[c] + k
            tr, ti = tw_ref[0, at : at + 1, :], tw_ref[1, at : at + 1, :]
            re, im = back[k, :, :LANES], back[k, :, LANES:]
            field[at, :, :LANES] = re * tr - im * ti
            field[at, :, LANES:] = im * tr + re * ti
        if twice:

            @pl.when(inner(me) == 1)
            def _():
                extra_copy(c).start()

    def extra_copy(c):
        at = pl.ds(starts[c], sizes[c])
        return pltpu.make_async_remote_copy(
            src_ref=field.at[at, pl.ds(half, half)], dst_ref=extra.at[at],
            send_sem=extra_send, recv_sem=extra_recv,
            device_id={"sub": facing(me)}, device_id_type=pl.DeviceIdType.MESH,
        )

    def turn_order(at):
        level, c = at
        return (GAP * level * outer / 32 + starts[c], level)

    def spectrum(c):
        lines = field[starts[c] : starts[c] + sizes[c]].reshape(sizes[c] * beams, 2 * LANES)
        values = transformed(lines, wf_ref)
        if c == 0:
            pl.semaphore_wait(barrier, n - 1)
        publish(0, c, values)

    loads[later + 1].wait()
    for c in range(AHEAD):
        spectrum(c)
    for load in loads[later + 2 : later + 6]:
        load.wait()
    write_card()
    for v in range(1, n):
        card_copy(v).start()
    write_columns()
    prepare(0)
    for c in range(chunks):
        stage(0, c)
        if c + AHEAD < chunks:
            spectrum(c + AHEAD)
    loads[later + 6].wait()
    ready = 1
    for level, c in sorted(((a, b) for a in range(1, final) for b in range(chunks)), key=turn_order):
        while ready <= (final if level == final - 1 else level):
            prepare(ready)
            ready += 1
        stage(level, c)
        if ready < final:
            prepare(ready)
            ready += 1

    for g in range(beams // 8):
        at = slice(g * 8, g * 8 + 8)
        lines = [(field[k, at, :LANES], field[k, at, LANES:]) for k in range(outer)]
        for q, pair in enumerate(butterflies(lines, 1)):
            for p in range(2):
                if groups == 1:
                    sendbuf[q // per, q % per, p, at] = pair[p]
                else:
                    field[q, at, p * LANES : (p + 1) * LANES] = pair[p]
    if groups > 1:
        for q in range(outer):
            for p in range(2):
                line = field[q, :, p * LANES : (p + 1) * LANES]
                for g in range(groups):
                    parts = [line[s * rows : (s + 1) * rows, g * width : (g + 1) * width] for s in range(groups)]
                    sendbuf[q * groups + g, 0, p] = jnp.concatenate(parts, axis=1)

    def turn_send_to(there, rows):
        lines = pl.ds(0, rows)
        pltpu.make_async_remote_copy(
            src_ref=sendbuf.at[there, :, :, lines], dst_ref=gathered.at[me, :, :, lines],
            send_sem=turn_send, recv_sem=turn_recv,
            device_id={"sub": there}, device_id_type=pl.DeviceIdType.MESH,
        ).start()

    for v in range(1, n):
        there = (me + v) % n
        if not twice:
            turn_send_to(there, rows)
            continue
        part = inner(me) * ((bit(final) + bit_of(there, final)) % 2)
        pl.when(part == 0)(functools.partial(turn_send_to, there, rows))
        pl.when(part == 1)(functools.partial(turn_send_to, there, half))

    def share_copy(slot, target):
        return pltpu.make_async_remote_copy(
            src_ref=packed.at[slot], dst_ref=gathered.at[facing(me), :, :, pl.ds(half, half)],
            send_sem=share_send, recv_sem=share_recv,
            device_id={"sub": target}, device_id_type=pl.DeviceIdType.MESH,
        )

    def shared(count):
        return all_of(packed.at[pl.ds(0, count)], packed.at[pl.ds(0, count)], share_send, share_recv)

    def turned_slabs(count):
        return all_of(sendbuf.at[pl.ds(0, count)], gathered.at[pl.ds(0, count)], turn_send, turn_recv)

    if twice:

        @pl.when(inner(me) == 1)
        def _():
            all_of(extra, extra, extra_send, extra_recv).wait_recv()
            lines = [(extra[k, :, :LANES], extra[k, :, LANES:]) for k in range(outer)]
            even, odd = butterflies(lines[0::2], 1), butterflies(lines[1::2], 1)
            sign = (1 - 2 * bit(final)).astype(F32)
            for k in range(outer // 2):
                angle = 2.0 * math.pi * k / outer
                turn = times_constant(odd[k], complex(math.cos(angle), math.sin(angle)))
                for p in range(2):
                    packed[k // per, k % per, p] = even[k][p] + sign * turn[p]

        for slot in range(n // 2):
            target = bit(final) * (n // 2) + slot
            pl.when(inner(me) * jnp.where(target == me, 0, 1) == 1)(share_copy(slot, target).start)

        @pl.when(inner(me) == 1)
        def _():
            gathered[facing(me), :, :, half:] = packed[me % (n // 2)]

    gathered[me] = sendbuf[me]
    cards[me] = card[...]
    all_of(cards.at[pl.ds(0, n - 2)], cards.at[pl.ds(0, n - 2)], card_send, card_recv).wait_recv()
    families = n // 16
    if groups == 1:
        lane = lax.broadcasted_iota(jnp.int32, (half, LANES), 1)
        for h in range(2):
            for g in range(families):
                tiles = []
                for side in range(2):
                    for f in range(8):
                        values = cards[h * (n // 2) + g * 8 + f]
                        child = side ^ h
                        moved = pltpu.roll(values, (f - child) * beams % LANES, 1)
                        tiles.append(jnp.where((lane >= f * beams) & (lane < (f + 1) * beams), moved, 0.0))
                high, low = split(jnp.concatenate(tiles, axis=0))
                more[h, g, 0] = high
                more[h, g, 1] = low
    for level in range(final):
        sent = state.at[level, 1 - bit(level)]
        all_of(sent, landed.at[level], level_send.at[level], level_recv.at[level, 0]).wait_send()
    all_of(cards.at[pl.ds(0, n - 1)], cards.at[pl.ds(0, n - 1)], card_send, card_recv).wait_send()
    if groups > 1:
        more[...] = cards[...]
    if not twice:
        turned_slabs(n - 1).wait_recv()
        turned_slabs(n - 1).wait_send()
        return
    turned_slabs(n - 1 - n // 16).wait_recv()

    @pl.when(inner(me) == 0)
    def _():
        shared(n // 8).wait_recv()
        turned_slabs(n - 1).wait_send()

    @pl.when(inner(me) == 1)
    def _():
        shared(n // 8 - 1).wait_recv()
        turned_slabs(n - 1 - n // 4).wait_send()
        shared(n // 2 - 1).wait_send()
        all_of(extra, extra, extra_send, extra_recv).wait_send()


def finish(cfg, gathered, last, out_hbm, out_ref, sem):
    n, per, half = cfg["n"], cfg["per"], cfg["beams"] // 2
    families = n // 16
    stores = []
    for r in range(per):
        for p in range(2):
            for h in range(2):
                for g in range(families):
                    sides = [
                        gathered[at : at + 8, r, p, h * half : (h + 1) * half].reshape(LANES // 2, LANES)
                        for at in (g * 8, n // 2 + g * 8)
                    ]
                    high, low = split(jnp.concatenate(sides, axis=0).T)
                    value = dot(high, last[h, g, 0]) + dot(low, last[h, g, 0]) + dot(high, last[h, g, 1])
                    at = (h * families + g) * LANES
                    out_ref[p, r * LANES : (r + 1) * LANES, at : at + LANES] = value
            at = (p, pl.ds(r * LANES, LANES))
            stores.append(pltpu.make_async_copy(out_ref.at[at], out_hbm.at[at], sem.at[r, p]))
            stores[-1].start()
    for store in stores:
        store.wait()


def real_form(length, direction, factor):
    index = np.arange(length)
    turns = (index[:, None] * index[None, :] % length) * (direction * 2.0 * np.pi / length)
    c, s = np.cos(turns) * factor, np.sin(turns) * factor
    full = np.block([[c, s], [-s, c]]).astype(np.float32)
    high = np.asarray(full, dtype=jnp.bfloat16)
    low = np.asarray(full - high.astype(np.float32), dtype=jnp.bfloat16)
    return np.stack([high, low])


def body(n, sub_images, shift_table, phase_table, offset_table, weight_table):
    beams, bins = sub_images.shape[1], sub_images.shape[2]
    levels, taps = shift_table.shape[0], weight_table.shape[3]
    outer = bins // LANES
    share = bins // n
    per = max(1, share // LANES)
    groups = max(1, LANES // share)
    sizes = tuple(part * outer // sum(CHUNKS) for part in CHUNKS)
    rows = beams // groups
    cfg = dict(n=n, levels=levels, outer=outer, beams=beams, sizes=sizes, per=per, groups=groups,
               width=min(share, LANES), rows=rows, taps=taps, twice=groups == 1 and levels > 2)
    turns = np.arange(outer)[:, None] * np.arange(LANES)[None, :] * (2.0 * np.pi / bins)
    twiddle = np.stack([np.cos(turns), np.sin(turns)]).astype(np.float32)
    half = beams // 2
    blocks = -(-levels * (6 + 2 * taps) // LANES)
    shapes = [((n, per, 2, rows, LANES), F32)]
    shapes.append(((2, n // 16, 2, LANES, LANES), BF16) if groups == 1 else ((n, half, LANES), F32))
    held = sum(math.prod(shape) * jnp.dtype(kind).itemsize for shape, kind in shapes)
    vmem = pl.BlockSpec(memory_space=pltpu.VMEM)
    operands = (
        sub_images, shift_table, phase_table, offset_table, weight_table, jnp.asarray(real_form(LANES, -1, 1.0)),
        jnp.asarray(real_form(LANES, 1, 1.0 / bins)), jnp.asarray(twiddle),
    )
    result = pl.pallas_call(
        functools.partial(kernel, cfg),
        name="merges",
        out_shape=[pltpu.VMEM(*shape) for shape in shapes],
        in_specs=[pl.BlockSpec(memory_space=pltpu.HBM)] * 8,
        out_specs=[vmem] * len(shapes),
        scratch_shapes=[
            *[pltpu.VMEM(a.shape, a.dtype) for a in operands],
            pltpu.VMEM((outer, beams, 2 * LANES), F32),
            pltpu.VMEM((levels - 1, 2, outer, half, 2 * LANES), F32),
            pltpu.VMEM((levels - 1, outer, half, 2 * LANES), F32),
            pltpu.VMEM((blocks * LANES, LANES), F32),
            pltpu.VMEM((blocks, LANES, LANES), F32),
            pltpu.VMEM((levels, 4, beams, LANES), F32),
            pltpu.VMEM((levels - 1, 2, max(sizes) * beams, max(sizes) * beams), BF16),
            pltpu.VMEM((n, per, 2, rows, LANES), F32),
            pltpu.VMEM((half, LANES), F32),
            pltpu.VMEM((n, half, LANES), F32),
            pltpu.VMEM((outer, half, 2 * LANES), F32),
            pltpu.VMEM((n // 2, per, 2, half, LANES), F32),
            pltpu.SemaphoreType.DMA((beams // 8 + 7,)),
            pltpu.SemaphoreType.DMA((levels - 1,)),
            pltpu.SemaphoreType.DMA((levels - 1, len(sizes))),
            pltpu.SemaphoreType.DMA((9,)),
        ],
        compiler_params=pltpu.CompilerParams(
            collective_id=0, has_side_effects=True, vmem_limit_bytes=VMEM - held
        ),
    )(*operands)
    if groups == 1:
        shape = (2, per * LANES, n * beams)
        return pl.pallas_call(
            functools.partial(finish, cfg),
            name="finish",
            out_shape=jax.ShapeDtypeStruct(shape, F32),
            in_specs=[vmem] * 2,
            out_specs=pl.BlockSpec(memory_space=pltpu.HBM),
            scratch_shapes=[pltpu.VMEM(shape, F32), pltpu.SemaphoreType.DMA((per, 2))],
            compiler_params=pltpu.CompilerParams(vmem_limit_bytes=24000000),
        )(*result)
    pieces = result[0].reshape(n, 2, rows, groups, share).transpose(1, 4, 0, 3, 2)
    pieces = pieces.reshape(2, share, 2, n // 2, 2, half)
    blocks = result[1][:, :, : 2 * beams].reshape(2, n // 2, half, 2, beams)
    sums = []
    for h in range(2):
        total = 0.0
        for child in range(2):
            total = total + jnp.einsum(
                "pqim,imj->pqij", pieces[:, :, h ^ child, :, h], blocks[h, :, :, child], precision=lax.Precision.HIGHEST
            )
        sums.append(total)
    return jnp.stack(sums, axis=2).reshape(2, share, n * beams)


def solution(mesh):
    placed = (
        P(None, ("img", "sub"), None),
        P(None, "sub", None, None),
        P(None, "sub", None, None),
        P(None, "sub", None, None),
        P(None, "sub", None, None, None),
    )
    return jax.shard_map(
        functools.partial(body, mesh.shape["sub"]),
        mesh=mesh, in_specs=placed, out_specs=P(None, ("img", "sub"), None), check_vma=False,
    )
```
